32 devices in a mesh: row: 4 (over z), col: 8 (over y, x, core).
Axes of the slice: x: 2, y: 2, z: 4, core: 2. Of those that a mesh axis runs over, the one named last changes fastest.
Arguments:
- pressure: float32 [128, 256, 512], P('row', 'col'), may hold values from -6 to 6
- cut_exponent: int32 [4, 8, 2], P('row', 'col'), may hold values from 0 to 3
- group_map: int32 [4, 8, 2], P('row', 'col'), may hold values from 0 to 15
Outputs:
- coeffs: float32 [128, 256, 512], P('row', 'col')
- group_mass: float32 [16, 4], replicated
The draws below stay inside these ranges and needn't reach their ends.
Inputs may be any that keep to these rules, and one draw needn't show every extreme that they name: `cut_exponent`: one exponent per block of 32 x 32 x 512 // 2 cells.
All inputs are finite; a program needn't handle non-finite values.
Results may differ from the reference program's by a relative error of at most 0.0001.
Values sent between devices are 32-bit elements; how exact they have to be, the bound alone decides.
A program may use at most 64 MiB of HBM per device.

```python
import jax
import jax.numpy as jnp
from jax import lax

CX = 32
CY = 32
CZ = 512
ZB = 2
GROUPS = 16
NX = 128
NY = 256
N_ROW = 4
N_COL = 8


def with_ends(entries, rng, low, largest):
    dims = entries.shape
    place = [jax.random.randint(jax.random.fold_in(rng, axis), (), 0, dims[axis]) for axis in range(len(dims))]
    entries = entries.at[tuple(place)].set(low)
    longest = dims.index(max(dims))
    place[longest] = (place[longest] + 1) % dims[longest]
    return entries.at[tuple(place)].set(largest)


def block_scale(rng, shape, cuts, low, largest):
    def one(axis_at, blocks):
        steps = jax.random.uniform(jax.random.fold_in(jax.random.fold_in(rng, 6), axis_at), (blocks,), jnp.float32, low / len(cuts), largest / len(cuts))
        return jnp.repeat(jnp.exp(steps), shape[axis_at] // blocks).reshape((-1,) + (1,) * (len(shape) - axis_at - 1))

    gain = one(*cuts[0])
    for cut in cuts[1:]:
        gain = gain * one(*cut)
    return gain


def bell_draw(stream_key, shape, spread, most, cuts=(), held_as=jnp.bfloat16):
    values = jax.random.normal(stream_key, shape, jnp.float32) * spread
    if len(cuts) > 0:
        values = block_scale(stream_key, shape, cuts, -0.22, 0.18) * values
    return jnp.clip(values, min=-most, max=most).astype(held_as)


def setup_inputs(seed: int = 0) -> dict:
    splits = jax.random.split(jax.random.key(seed), 4)
    pressure = bell_draw(splits[0], (NX, NY, CZ), 1.0, 6.0, ((0, 4), (1, 8)), jnp.float32)
    cut_exponent = with_ends(jax.random.randint(splits[1], (N_ROW, N_COL, ZB), 0, 4), jax.random.fold_in(splits[1], 1), 0, 3).astype(jnp.int32)
    group_map = with_ends(jax.random.randint(splits[2], (N_ROW, N_COL, ZB), 0, GROUPS), jax.random.fold_in(splits[2], 1), 0, GROUPS - 1).astype(jnp.int32)
    return dict(pressure=pressure, cut_exponent=cut_exponent, group_map=group_map)


cut_levels = (0.25, 0.5, 1.0, 2.0)


def lift_axis(signal, axis_pos):
    length = signal.shape[axis_pos]
    evens_half = lax.slice_in_dim(signal, 0, length, stride=2, axis=axis_pos)
    odds_half = lax.slice_in_dim(signal, 1, length, stride=2, axis=axis_pos)
    guess = 0.5625 * (evens_half + jnp.roll(evens_half, -1, axis_pos)) - 0.0625 * (jnp.roll(evens_half, 1, axis_pos) + jnp.roll(evens_half, -2, axis_pos))
    detail = odds_half - guess
    smooth = evens_half + (0.28125 * (jnp.roll(detail, 1, axis_pos) + detail) - 0.03125 * (jnp.roll(detail, 2, axis_pos) + jnp.roll(detail, -1, axis_pos)))
    return jnp.stack([smooth, detail], axis_pos + 1).reshape(signal.shape)


def reference(pressure, cut_exponent, group_map):
    coeffs = lift_axis(pressure, 0)
    coeffs = lift_axis(coeffs, 1)
    coeffs = lift_axis(coeffs, 2)
    parity_x = (jnp.arange(NX, dtype=jnp.int32) % 2)[:, None, None]
    parity_y = (jnp.arange(NY, dtype=jnp.int32) % 2)[None, :, None]
    parity_z = (jnp.arange(CZ, dtype=jnp.int32) % 2)[None, None, :]
    detail_mask = (parity_x + parity_y + parity_z) > 0
    magnitude = jnp.where(detail_mask, jnp.abs(coeffs), jnp.float32(0.0))
    shaped = magnitude.reshape(N_ROW, CX, N_COL, CY, ZB, CZ // ZB)
    scales = jnp.exp2(-cut_exponent.astype(jnp.float32))
    cells = CX * CY * (CZ // ZB)
    block_list = []
    for level_value in cut_levels:
        limit = (level_value * scales)[:, None, :, None, :, None]
        block_list.append(jnp.sum(jnp.maximum(shaped - limit, 0.0), axis=(1, 3, 5)) / cells)
    block_mass = jnp.stack(block_list, -1)
    onehot = (group_map[..., None] == jnp.arange(GROUPS, dtype=jnp.int32)).astype(jnp.float32)
    group_mass = jnp.einsum("abzg,abzk->gk", onehot, block_mass.astype(jnp.float32), precision=lax.Precision.HIGHEST)
    return coeffs, group_mass
```

```python
import functools

import jax
import jax.numpy as jnp
import numpy as np
from jax import lax
from jax.experimental import pallas as pl
from jax.experimental.pallas import tpu as pltpu
from jax.sharding import PartitionSpec as P

GROUPS = 16
LEVELS = (0.25, 0.5, 1.0, 2.0)
MESH = pl.DeviceIdType.MESH
F32, BF16 = jnp.float32, jnp.bfloat16
TILE, LANES = 8, 128
UNROLL = 64


def cyclic_matrix(n):
    ev, od = np.eye(n)[0::2], np.eye(n)[1::2]
    r = lambda a, k: np.roll(a, k, 0)
    d = od - (0.5625 * (ev + r(ev, -1)) - 0.0625 * (r(ev, 1) + r(ev, -2)))
    s = ev + (0.28125 * (r(d, 1) + d) - 0.03125 * (r(d, 2) + r(d, -1)))
    return np.stack([s, d], 1).reshape(n, n)


def local_matrix(n):
    half = n // 2
    t = np.eye(n + 6)
    v, (a, b, c, f0, f1, g) = t[:n], t[n:]
    e = {j: v[2 * j] for j in range(half)}
    o = {j: v[2 * j + 1] for j in range(half)}
    e[-1], e[half], e[half + 1] = a, f0, f1
    d = {
        j: o[j] - 0.5625 * (e[j] + e[j + 1]) + 0.0625 * (e[j - 1] + e[j + 2])
        for j in range(half)
    }
    d[-1] = b - 0.5625 * e[0] + 0.0625 * e[1]
    d[-2] = c + 0.0625 * e[0]
    d[half] = g + 0.0625 * e[half - 1]
    out = np.zeros((n, n + 6))
    for j in range(half):
        out[2 * j] = e[j] + 0.28125 * (d[j - 1] + d[j]) - 0.03125 * (d[j - 2] + d[j + 1])
        out[2 * j + 1] = d[j]
    return out


def partials_low(row, n):
    a = row(n - 2)
    b = row(n - 1) - 0.5625 * a + 0.0625 * row(n - 4)
    c = row(n - 3) - 0.5625 * (row(n - 4) + a) + 0.0625 * row(n - 6)
    return a, b, c


def partials_high(row):
    f0, f1 = row(0), row(2)
    return f0, f1, row(1) - 0.5625 * (f0 + f1) + 0.0625 * row(4)


def split(value):
    hi = value.astype(BF16)
    return hi, (value - hi.astype(F32)).astype(BF16)


def dot2(left, right):
    dot = functools.partial(jnp.dot, preferred_element_type=F32)
    if left.dtype == BF16:
        hi, lo = split(right)
        return dot(left, hi) + dot(left, lo)
    hi, lo = split(left)
    return dot(hi, right) + dot(lo, right)


def doublings(n_row, n_col):
    hops, known = [], 1
    while known < n_col // 2:
        hops.append((1, known))
        known *= 2
    known = 0
    while known < n_row // 2:
        hops.append((0, max(known, 1)))
        known += max(known, 1)
    return hops


def kernel(n_row, n_col, grp, cut_hbm, map_hbm, p_ref, *refs):
    weights, refs = refs[:8], refs[8:]
    out_ref, mass_ref = refs[:2]
    ext, v, q, hs, h, su, u, sc, cb, part, slots, cut_ref, map_ref = refs[2:15]
    held = refs[15:23]
    ws_ref, wz_ref, wy_ref, wu_ref, wsa_ref, wxa_ref, wxb_ref, wc_ref = held
    in_sem, w_sem, h_send, h_recv, g_send, g_recv, hop_sem = refs[23:]
    nx, ny, nz = p_ref.shape
    half = nx // 2
    devices = n_row * n_col
    row, col = lax.axis_index("row"), lax.axis_index("col")
    me = row * n_col + col
    away_r = lambda k: lax.rem(row + (k + n_row), n_row)
    away_c = lambda k: lax.rem(col + (k + n_col), n_col)
    up_r, dn_r, up_c, dn_c = away_r(1), away_r(-1), away_c(1), away_c(-1)

    barrier = pltpu.get_barrier_semaphore()
    for r, c in ((up_r, col), (dn_r, col), (row, up_c), (row, dn_c)):
        pl.semaphore_signal(barrier, inc=1, device_id=(r, c), device_id_type=MESH)

    loads = []
    starts = [0, nx - grp, *range(grp, nx - grp, grp)]
    for i, at in enumerate(starts):
        load = pltpu.make_async_copy(
            p_ref.at[pl.ds(at, grp)], ext.at[pl.ds(at, grp)], in_sem.at[i]
        )
        load.start()
        loads.append(load)
    fetched = []
    for i, (src, dst) in enumerate(
        zip((*weights, cut_hbm, map_hbm), (*held, cut_ref, map_ref), strict=True)
    ):
        fetch = pltpu.make_async_copy(src, dst, w_sem.at[i])
        fetch.start()
        fetched.append(fetch)

    hops = doublings(n_row, n_col)

    def call(k):
        axis, far = hops[k]
        if axis:
            aim = ((row, away_c(far)), (row, away_c(-far)))
        else:
            aim = ((away_r(far), col), (away_r(-far), col))
        for to in aim:
            pl.semaphore_signal(hop_sem.at[k], inc=1, device_id=to, device_id_type=MESH)

    def relay(k):
        if k < len(hops):
            pl.semaphore_wait(hop_sem.at[k], 2)
            if k + 1 < len(hops):
                call(k + 1)

    sends = []

    def send(src, dst, to):
        i = len(sends)
        copy = pltpu.make_async_remote_copy(
            src_ref=src, dst_ref=dst, send_sem=h_send.at[i], recv_sem=h_recv.at[i],
            device_id=to, device_id_type=MESH,
        )
        copy.start()
        sends.append(copy)
        return copy

    with jax.named_scope("ld01"):
        loads[0].wait()
        loads[1].wait()
    with jax.named_scope("hs"):
        for i, plane in enumerate(partials_low(lambda i: ext[i], nx) + partials_high(lambda i: ext[i])):
            hs[i] = plane
    with jax.named_scope("bar"):
        pl.semaphore_wait(barrier, 4)
    lo, hi = pl.ds(0, 3), pl.ds(3, 3)
    outer, inner = [], []
    for rows, kept in (
        (pl.ds(0, TILE), outer), (pl.ds(ny - TILE, TILE), outer),
        (pl.ds(TILE, ny - 2 * TILE), inner),
    ):
        kept.append(send(hs.at[lo, rows], h.at[lo, rows], (up_r, col)))
        kept.append(send(hs.at[hi, rows], h.at[hi, rows], (dn_r, col)))
    if hops:
        call(0)

    with jax.named_scope("su"):
        fetched[0].wait()
        near = []
        for i, at in enumerate(starts):
            if i > 1:
                loads[i].wait()
            at = pl.ds(at, grp)
            got = dot2(ws_ref[...], ext[at].reshape(grp * ny, nz))
            su[:, at, :] = got.reshape(6, grp, nz)
            near.append(send(su.at[lo, at], u.at[lo, at], (row, up_c)))
            near.append(send(su.at[hi, at], u.at[hi, at], (row, dn_c)))
    relay(0)
    groups = nx // grp
    with jax.named_scope("z"):
        fetched[1].wait()
        for g in range(groups):
            at = pl.ds(g * grp, grp)
            v[at] = dot2(ext[at].reshape(grp * ny, nz), wz_ref[...]).reshape(grp, ny, nz)
            if g == groups // 2 - 1:
                relay(1)
    relay(2)
    with jax.named_scope("y"):
        for fetch in fetched[2:]:
            fetch.wait()
        for g in range(groups):
            at = pl.ds(g * grp, grp)
            q[at] = dot2(wy_ref[...], v[at].reshape(grp * ny, nz)).reshape(grp, ny, nz)
    relay(3)
    with jax.named_scope("wait_u"):
        for copy in near:
            copy.wait_recv()
    with jax.named_scope("u"):
        zu = dot2(u[...].reshape(6 * nx, nz), wz_ref[...]).reshape(6, nx, nz)
        for g in range(groups):
            at = slice(g * grp, (g + 1) * grp)
            more = dot2(wu_ref[...], zu[:, at, :].reshape(6 * grp, nz))
            q[at] += more.reshape(grp, ny, nz)
    for k in range(4, len(hops)):
        relay(k)

    zb = cut_ref.shape[2]
    width = nz // zb
    n_lev = len(LEVELS)
    odd = lambda axis: lax.broadcasted_iota(jnp.int32, (TILE, LANES), axis) % 2
    mixed = (odd(0) + odd(1)) > 0

    def x_stage(totals, edges):
        totals = list(totals)
        for z in range(zb):
            cuts = jnp.full((TILE, LANES), -cut_ref[0, 0, z], jnp.int32)
            scale = jnp.exp2(cuts.astype(F32))
            limits = [level * scale for level in LEVELS]

            def tile(t, sums, z=z, limits=limits):
                rows = pl.ds(pl.multiple_of(t * TILE, TILE), TILE)
                sums = list(sums)
                for at in range(z * width, (z + 1) * width, LANES):
                    lanes = pl.ds(at, LANES)

                    def put(plane, value):
                        out_ref[plane, rows, lanes] = value
                        size = jnp.abs(value)
                        if plane % 2 == 0:
                            size = jnp.where(mixed, size, 0.0)
                        for n, limit in enumerate(limits):
                            sums[n] += jnp.maximum(size - limit, 0.0)

                    far = {-1: nx, half: nx + 3, half + 1: nx + 4}
                    e = lambda j: q[far.get(j, 2 * j), rows, lanes]

                    def detail(j):
                        if j == -1:
                            return q[nx + 1, rows, lanes] - 0.5625 * e(0) + 0.0625 * e(1)
                        if j == -2:
                            return q[nx + 2, rows, lanes] + 0.0625 * e(0)
                        if j == half:
                            return q[nx + 5, rows, lanes] + 0.0625 * e(half - 1)
                        return q[2 * j + 1, rows, lanes] - 0.5625 * (e(j) + e(j + 1)) + 0.0625 * (e(j - 1) + e(j + 2))

                    def smooth(d, j):
                        put(2 * j, e(j) + 0.28125 * (d[j - 1] + d[j]) - 0.03125 * (d[j - 2] + d[j + 1]))

                    if not edges:
                        d = {}
                        for j in range(1, half - 2):
                            d[j] = detail(j)
                            put(2 * j + 1, d[j])
                            if j >= 4:
                                smooth(d, j - 1)
                    else:
                        d = {j: out_ref[2 * j + 1, rows, lanes] for j in (1, 2, 3)}
                        d |= {j: detail(j) for j in (-2, -1, 0)}
                        put(1, d[0])
                        for j in (0, 1, 2):
                            smooth(d, j)
                        d = {j: out_ref[2 * j + 1, rows, lanes] for j in range(half - 5, half - 2)}
                        d |= {j: detail(j) for j in range(half - 2, half + 1)}
                        for j in (half - 2, half - 1):
                            put(2 * j + 1, d[j])
                        for j in range(half - 3, half):
                            smooth(d, j)
                return tuple(sums)

            mine = slice(z * n_lev, (z + 1) * n_lev)
            totals[mine] = lax.fori_loop(0, ny // TILE, tile, tuple(totals[mine]))
        return totals

    with jax.named_scope("wait_outer"):
        for copy in outer:
            copy.wait_recv()
    with jax.named_scope("corner"):
        rim = jnp.concatenate([h[:, :TILE, :], h[:, ny - TILE :, :]], 1).reshape(12 * TILE, nz)
        zrim = dot2(rim, wz_ref[...])
        sc[...] = dot2(wsa_ref[...], zrim).reshape(6, TILE, nz)
        corner = [
            send(sc.at[lo], cb.at[lo], (row, up_c)),
            send(sc.at[hi], cb.at[hi], (row, dn_c)),
        ]
        q[pl.ds(nx, 6)] = dot2(wxa_ref[...], zrim).reshape(6, ny, nz)
    with jax.named_scope("xin"):
        totals = [jnp.zeros((TILE, LANES), F32) for _ in range(zb * n_lev)]
        totals = x_stage(totals, False)
    with jax.named_scope("wait_inner"):
        for copy in inner:
            copy.wait_recv()
    with jax.named_scope("wait_corner"):
        for copy in corner:
            copy.wait_recv()
    with jax.named_scope("edge"):
        core = h[:, TILE : ny - TILE, :].reshape(6 * (ny - 2 * TILE), nz)
        edge = dot2(wxb_ref[...], dot2(core, wz_ref[...]))
        edge += dot2(wc_ref[...], cb[...].reshape(6 * TILE, nz))
        q[pl.ds(nx, 6)] += edge.reshape(6, ny, nz)
    with jax.named_scope("xedge"):
        totals = x_stage(totals, True)
    with jax.named_scope("line"):
        lane = lax.broadcasted_iota(jnp.int32, (1, LANES), 1)
        line = jnp.zeros((1, LANES), F32)
        cells = nx * ny * width
        for z in range(zb):
            for n in range(n_lev):
                mass = jnp.sum(totals[z * n_lev + n], keepdims=True) / cells
                line += jnp.where(lane == n * GROUPS + map_ref[0, 0, z], mass, 0.0)
        part[...] = line
        slots[me] = line

    def spread(r, c, t):
        return pltpu.make_async_remote_copy(
            src_ref=part, dst_ref=slots.at[me], send_sem=g_send.at[t],
            recv_sem=g_recv.at[me], device_id=(r, c), device_id_type=MESH,
        )

    def gather(r, c, t):
        return pltpu.make_async_remote_copy(
            src_ref=part, dst_ref=slots.at[t], send_sem=g_send.at[t],
            recv_sem=g_recv.at[t], device_id=(r, c), device_id_type=MESH,
        )

    def peers(visit):
        if devices <= UNROLL:
            for j in reversed(range(n_row)):
                for k in range(n_col):
                    if j or k:
                        r, c = away_r(j), away_c(k)
                        visit(r, c, r * n_col + c)
            return

        @pl.loop(1, n_row)
        def _(j):
            @pl.loop(0, n_col)
            def _(k):
                r, c = lax.rem(row + j, n_row), lax.rem(col + k, n_col)
                visit(r, c, r * n_col + c)

        @pl.loop(1, n_col)
        def _(k):
            c = lax.rem(col + k, n_col)
            visit(row, c, row * n_col + c)

    with jax.named_scope("spread"):
        peers(lambda r, c, t: spread(r, c, t).start())
    with jax.named_scope("wsend"):
        for copy in sends:
            copy.wait_send()
    with jax.named_scope("gather"):
        peers(lambda r, c, t: gather(r, c, t).wait())
    with jax.named_scope("sum"):
        total = jnp.sum(slots[...], axis=0)
        mass_ref[...] = jnp.concatenate(
            [total[:, n * GROUPS : (n + 1) * GROUPS] for n in range(n_lev)], 0
        )


def deliver(c_ref, m_ref, out_hbm, mass_hbm, sems, m_sem):
    count = sems.shape[0]
    size = c_ref.shape[0] // count
    copies = [pltpu.make_async_copy(m_ref, mass_hbm, m_sem)]
    for i in range(count):
        at = pl.ds(i * size, size)
        copies.append(pltpu.make_async_copy(c_ref.at[at], out_hbm.at[at], sems.at[i]))
    for copy in copies:
        copy.start()
    for copy in copies:
        copy.wait()


def solution(mesh):
    n_row, n_col = mesh.shape["row"], mesh.shape["col"]

    def shards(pressure, cut_exponent, group_map):
        nx, ny, nz = pressure.shape
        grp = 8
        devices = n_row * n_col
        local = local_matrix(ny)
        own, beyond = local[:, :ny], local[:, ny:]
        wy = np.kron(np.eye(grp), own)
        wu = np.einsum("xw,yk->xykw", np.eye(grp), beyond).reshape(grp * ny, 6 * grp)
        eye = np.eye(ny)
        take = lambda i: eye[i]
        near = np.stack(partials_low(take, ny) + partials_high(take))
        ws = np.einsum("ky,xw->kxwy", near, np.eye(grp)).reshape(6 * grp, grp * ny)
        rim = np.r_[0:TILE, ny - TILE : ny]
        six = np.eye(6, TILE).T
        wsa = np.einsum("ky,wp->kwpy", near[:, rim], six).reshape(6 * TILE, 6 * 2 * TILE)
        wxa = np.kron(np.eye(6), own[:, rim])
        wxb = np.kron(np.eye(6), own[:, TILE : ny - TILE])
        wc = np.einsum("wp,yk->pykw", six, beyond).reshape(6 * ny, 6 * TILE)
        weights = [
            jnp.asarray(w, BF16)
            for w in (ws, cyclic_matrix(nz).T, wy, wu, wsa, wxa, wxb, wc)
        ]
        vmem = pl.BlockSpec(memory_space=pltpu.VMEM)
        hbm = pl.BlockSpec(memory_space=pltpu.HBM)
        hops = len(doublings(n_row, n_col))
        n_sends = 6 + 2 * (nx // grp) + 2
        found = pl.pallas_call(
            functools.partial(kernel, n_row, n_col, grp),
            out_shape=(
                pltpu.VMEM((nx, ny, nz), F32),
                pltpu.VMEM((len(LEVELS), GROUPS), F32),
            ),
            in_specs=[hbm] * (3 + len(weights)),
            out_specs=(vmem, vmem),
            scratch_shapes=[
                pltpu.VMEM((nx, ny, nz), F32),
                pltpu.VMEM((nx, ny, nz), F32),
                pltpu.VMEM((nx + 6, ny, nz), F32),
                pltpu.VMEM((6, ny, nz), F32),
                pltpu.VMEM((6, ny, nz), F32),
                pltpu.VMEM((6, nx, nz), F32),
                pltpu.VMEM((6, nx, nz), F32),
                pltpu.VMEM((6, TILE, nz), F32),
                pltpu.VMEM((6, TILE, nz), F32),
                pltpu.VMEM((1, LANES), F32),
                pltpu.VMEM((devices, 1, LANES), F32),
                pltpu.SMEM(cut_exponent.shape, jnp.int32),
                pltpu.SMEM(group_map.shape, jnp.int32),
                *(pltpu.VMEM(w.shape, BF16) for w in weights),
                pltpu.SemaphoreType.DMA((nx // grp,)),
                pltpu.SemaphoreType.DMA((len(weights) + 2,)),
                pltpu.SemaphoreType.DMA((n_sends,)),
                pltpu.SemaphoreType.DMA((n_sends,)),
                pltpu.SemaphoreType.DMA((devices,)),
                pltpu.SemaphoreType.DMA((devices,)),
                pltpu.SemaphoreType.REGULAR((max(hops, 1),)),
            ],
            compiler_params=pltpu.CompilerParams(
                collective_id=0, has_side_effects=True, vmem_limit_bytes=24 * 2**20
            ),
        )(*(pltpu.with_memory_space_constraint(x, pltpu.HBM) for x in (cut_exponent, group_map, pressure, *weights)))
        coeffs, mass = pl.pallas_call(
            deliver,
            out_shape=tuple(pltpu.HBM(f.shape, F32) for f in found),
            in_specs=[vmem] * 2,
            out_specs=(hbm, hbm),
            scratch_shapes=[pltpu.SemaphoreType.DMA((8,)), pltpu.SemaphoreType.DMA],
            compiler_params=pltpu.CompilerParams(vmem_limit_bytes=2**20),
        )(*(pltpu.with_memory_space_constraint(x, pltpu.VMEM) for x in found))
        return coeffs, mass.T

    specs = P("row", "col", None)
    return jax.shard_map(
        shards, mesh=mesh, in_specs=(specs,) * 3, out_specs=(specs, P()), check_vma=False
    )
```

```python
import functools

import jax
import jax.numpy as jnp
import numpy as np
from jax import lax
from jax.experimental import pallas as pl
from jax.experimental.pallas import tpu as pltpu
from jax.sharding import PartitionSpec as P

GROUPS = 16
LEVELS = (0.25, 0.5, 1.0, 2.0)
MESH = pl.DeviceIdType.MESH
F32, BF16 = jnp.float32, jnp.bfloat16
TILE, LANES = 8, 128
UNROLL = 64


def cyclic_matrix(n):
    ev, od = np.eye(n)[0::2], np.eye(n)[1::2]
    r = lambda a, k: np.roll(a, k, 0)
    d = od - (0.5625 * (ev + r(ev, -1)) - 0.0625 * (r(ev, 1) + r(ev, -2)))
    s = ev + (0.28125 * (r(d, 1) + d) - 0.03125 * (r(d, 2) + r(d, -1)))
    return np.stack([s, d], 1).reshape(n, n)


def local_matrix(n):
    half = n // 2
    t = np.eye(n + 6)
    v, (a, b, c, f0, f1, g) = t[:n], t[n:]
    e = {j: v[2 * j] for j in range(half)}
    o = {j: v[2 * j + 1] for j in range(half)}
    e[-1], e[half], e[half + 1] = a, f0, f1
    d = {
        j: o[j] - 0.5625 * (e[j] + e[j + 1]) + 0.0625 * (e[j - 1] + e[j + 2])
        for j in range(half)
    }
    d[-1] = b - 0.5625 * e[0] + 0.0625 * e[1]
    d[-2] = c + 0.0625 * e[0]
    d[half] = g + 0.0625 * e[half - 1]
    out = np.zeros((n, n + 6))
    for j in range(half):
        out[2 * j] = e[j] + 0.28125 * (d[j - 1] + d[j]) - 0.03125 * (d[j - 2] + d[j + 1])
        out[2 * j + 1] = d[j]
    return out


def partials_low(row, n):
    a = row(n - 2)
    b = row(n - 1) - 0.5625 * a + 0.0625 * row(n - 4)
    c = row(n - 3) - 0.5625 * (row(n - 4) + a) + 0.0625 * row(n - 6)
    return a, b, c


def partials_high(row):
    f0, f1 = row(0), row(2)
    return f0, f1, row(1) - 0.5625 * (f0 + f1) + 0.0625 * row(4)


def split(value):
    hi = value.astype(BF16)
    return hi, (value - hi.astype(F32)).astype(BF16)


def dot2(left, right):
    dot = functools.partial(jnp.dot, preferred_element_type=F32)
    if left.dtype == BF16:
        hi, lo = split(right)
        return dot(left, hi) + dot(left, lo)
    hi, lo = split(left)
    return dot(hi, right) + dot(lo, right)


def dot_pair(left, right):
    return jnp.dot(left, jnp.concatenate(split(right), 0), preferred_element_type=F32)


def doublings(n_row, n_col):
    hops, known = [], 1
    while known < n_col // 2:
        hops.append((1, known))
        known *= 2
    known = 0
    while known < n_row // 2:
        hops.append((0, max(known, 1)))
        known += max(known, 1)
    return hops


def band(first_row, coefs):
    shape = (2 * TILE, LANES)
    lane = lax.broadcasted_iota(jnp.int32, shape, 1)
    far = jnp.abs(lane - lax.broadcasted_iota(jnp.int32, shape, 0) + first_row)
    value = jnp.zeros(shape, F32)
    for k, (even, odd) in enumerate(coefs):
        if even or odd:
            value = jnp.where(far == k, jnp.where(lane % 2 == 1, odd, even), value)
    return value.astype(BF16)


def fill_cyclic(ref):
    n = ref.shape[0]
    full = cyclic_matrix(n)
    reach = 7
    coefs = [(float(full[0, k]), float(full[1, 1 + k])) for k in range(reach)]
    made = {}
    for r in range(0, n, 2 * TILE):
        for c in range(0, n, LANES):
            off = (c - r + n // 2) % n - n // 2
            near = off - 2 * TILE < reach and off + LANES > -reach
            key = off if near else None
            if key not in made:
                made[key] = band(off, coefs) if near else jnp.zeros((2 * TILE, LANES), BF16)
            ref[pl.ds(r, 2 * TILE), pl.ds(c, LANES)] = made[key]


def kernel(n_row, n_col, grp, cut_hbm, map_hbm, p_ref, *refs):
    weights, refs = refs[:4], refs[4:]
    out_ref, mass_ref = refs[:2]
    ext, q, hs, yh, sh, ch, su, u, part, slots, cut_ref, map_ref, wz_ref = refs[2:15]
    held = refs[15:19]
    wx_ref, wy_ref, wc_ref, wu_ref = held
    in_sem, w_sem, h_send, h_recv, g_send, g_recv, hop_sem = refs[19:]
    nx, ny, nz = p_ref.shape
    half = nx // 2
    devices = n_row * n_col
    row, col = lax.axis_index("row"), lax.axis_index("col")
    me = row * n_col + col
    away_r = lambda k: lax.rem(row + (k + n_row), n_row)
    away_c = lambda k: lax.rem(col + (k + n_col), n_col)
    up_r, dn_r, up_c, dn_c = away_r(1), away_r(-1), away_c(1), away_c(-1)

    barrier = pltpu.get_barrier_semaphore()
    for r, c in ((up_r, col), (dn_r, col), (row, up_c), (row, dn_c)):
        pl.semaphore_signal(barrier, inc=1, device_id=(r, c), device_id_type=MESH)

    loads = []

    def load(at, size):
        i = len(loads)
        at = pl.ds(at, size)
        loads.append(pltpu.make_async_copy(p_ref.at[at], ext.at[at], in_sem.at[i]))
        loads[i].start()

    fetched = [
        pltpu.make_async_copy(src, dst, w_sem.at[i])
        for i, (src, dst) in enumerate(
            zip((*weights, cut_hbm, map_hbm), (*held, cut_ref, map_ref), strict=True)
        )
    ]
    for at in (*range(nx - 6, nx), *range(5)):
        load(at, 1)
    fetched[0].start()

    hops = doublings(n_row, n_col)

    def call(k):
        axis, far = hops[k]
        if axis:
            aim = ((row, away_c(far)), (row, away_c(-far)))
        else:
            aim = ((away_r(far), col), (away_r(-far), col))
        for to in aim:
            pl.semaphore_signal(hop_sem.at[k], inc=1, device_id=to, device_id_type=MESH)

    def relay(k):
        if k < len(hops):
            with jax.named_scope(f"r{k}"):
                pl.semaphore_wait(hop_sem.at[k], 2)
                if k + 1 < len(hops):
                    call(k + 1)

    sends = []

    def remote(i, src, dst, to):
        return pltpu.make_async_remote_copy(
            src_ref=src, dst_ref=dst, send_sem=h_send.at[i], recv_sem=h_recv.at[i],
            device_id=to, device_id_type=MESH,
        )

    def send(src, dst, to):
        copy = remote(len(sends), src, dst, to)
        copy.start()
        sends.append(copy)
        return copy

    def halo(piece, way):
        if isinstance(piece, int) and piece == 0:
            rows = pl.ds(TILE, ny - 2 * TILE)
        else:
            rows = pl.ds(pl.multiple_of((piece - 1) * (ny - TILE), TILE), TILE)
        three = lambda at: pl.ds(at + 3 * way, 3)
        to = lax.rem(row + 1 + way * (n_row - 2), n_row)
        return remote(
            2 + 2 * piece + way, yh.at[three(0), rows], q.at[three(nx), rows], (to, col)
        )

    with jax.named_scope("wz"):
        fill_cyclic(wz_ref)
        sh[:, pl.ds(6, TILE - 6), :] = jnp.zeros((6, TILE - 6, nz), F32)
    with jax.named_scope("ld01"):
        for copy in loads:
            copy.wait()
        fetched[0].wait()
    edges = len(loads)
    mid = nx - 11
    third = mid // 3
    for at in range(3):
        load(5 + at * third, third if at < 2 else mid - 2 * third)
    for fetch in fetched[1:]:
        fetch.start()
    with jax.named_scope("hs"):
        planes = partials_low(lambda i: ext[i], nx) + partials_high(lambda i: ext[i])
        for i, plane in enumerate(planes):
            hs[i] = plane
            line = lambda j: plane[j : j + 1]
            for k, one in enumerate(partials_low(line, ny) + partials_high(line)):
                sh[k, pl.ds(i, 1), :] = one
    lo, hi = pl.ds(0, 3), pl.ds(3, 3)
    odd_core = lax.rem(col, 2)
    is_last = (row == n_row - 1).astype(jnp.int32)
    is_first = (row == 0).astype(jnp.int32)
    far = is_first + (1 - is_first) * (1 - is_last) * odd_core
    ways = (far + odd_core - 2 * far * odd_core, 1 - (far + odd_core - 2 * far * odd_core))
    tail = (
        (1, ways[0]), (2 - odd_core, far),
        (1 + odd_core, odd_core * far + (1 - odd_core) * (1 - far)), (2, 1 - far),
    )

    outer_rows = (pl.ds(0, TILE), pl.ds(ny - TILE, TILE))

    def lift(way):
        three = pl.ds(3 * way, 3)
        lifted = dot2(hs[three].reshape(3 * ny, nz), wz_ref[...])
        yh[three] = dot_pair(wx_ref[...], lifted).reshape(3, ny, nz)

    with jax.named_scope("lift0"):
        lift(ways[0])
    with jax.named_scope("bar"):
        pl.semaphore_wait(barrier, 4)
    corner = [
        send(sh.at[lo], ch.at[lo], (row, up_c)),
        send(sh.at[hi], ch.at[hi], (row, dn_c)),
    ]
    inner, *outer = [[halo(piece, way) for way in range(2)] for piece in range(3)]
    sends.extend(inner + outer[0] + outer[1])
    halo(0, ways[0]).start()
    if hops:
        call(0)
    with jax.named_scope("lift1"):
        lift(ways[1])
    halo(0, ways[1]).start()

    groups = nx // grp
    near = {}

    def z_group(g):
        at = pl.ds(g * grp, grp)
        v = dot2(ext[at].reshape(grp * ny, nz), wz_ref[...])
        got = dot2(wy_ref[...], v)
        q[at] = got[: grp * ny].reshape(grp, ny, nz)
        su[:, at, :] = got[grp * ny :].reshape(6, grp, nz)
        near[g] = (
            send(su.at[lo, at], u.at[lo, at], (row, up_c)),
            send(su.at[hi, at], u.at[hi, at], (row, dn_c)),
        )

    with jax.named_scope("ld2"):
        for copy in loads[edges:]:
            copy.wait()
        for fetch in fetched[1:]:
            fetch.wait()
    order = (0, groups - 1, *range(1, groups - 1))
    with jax.named_scope("z"):
        for g in order[: groups // 2]:
            z_group(g)
    relay(0)
    with jax.named_scope("z2"):
        z_group(order[groups // 2])
    with jax.named_scope("wait_corner"):
        for copy in corner:
            copy.wait_recv()
    with jax.named_scope("outer"):
        lifted = dot2(ch[...].reshape(6 * TILE, nz), wz_ref[...])
        more = dot_pair(wc_ref[...], lifted).reshape(6, 2 * TILE, nz)
        for k, rows in enumerate(outer_rows):
            yh[:, rows, :] += more[:, k * TILE : (k + 1) * TILE, :]
        for piece, way in tail:
            halo(piece, way).start()
    with jax.named_scope("z3"):
        for g in order[groups // 2 + 1 :]:
            z_group(g)
    relay(1)

    zb = cut_ref.shape[2]
    width = nz // zb
    n_lev = len(LEVELS)
    odd = lambda axis: lax.broadcasted_iota(jnp.int32, (TILE, LANES), axis) % 2
    mixed = (odd(0) + odd(1)) > 0

    def x_stage(totals, edges, first, last):
        totals = list(totals)
        for z in range(zb):
            cuts = jnp.full((TILE, LANES), -cut_ref[0, 0, z], jnp.int32)
            scale = jnp.exp2(cuts.astype(F32))
            limits = [level * scale for level in LEVELS]

            def tile(t, sums, z=z, limits=limits):
                rows = pl.ds(pl.multiple_of(t * TILE, TILE), TILE)
                sums = list(sums)
                for at in range(z * width, (z + 1) * width, LANES):
                    lanes = pl.ds(at, LANES)

                    def put(plane, value):
                        out_ref[plane, rows, lanes] = value
                        size = jnp.abs(value)
                        if plane % 2 == 0:
                            size = jnp.where(mixed, size, 0.0)
                        for n, limit in enumerate(limits):
                            sums[n] += jnp.maximum(size - limit, 0.0)

                    far = {-1: nx, half: nx + 3, half + 1: nx + 4}
                    e = lambda j: q[far.get(j, 2 * j), rows, lanes]

                    def detail(j):
                        if j == -1:
                            return q[nx + 1, rows, lanes] - 0.5625 * e(0) + 0.0625 * e(1)
                        if j == -2:
                            return q[nx + 2, rows, lanes] + 0.0625 * e(0)
                        if j == half:
                            return q[nx + 5, rows, lanes] + 0.0625 * e(half - 1)
                        return q[2 * j + 1, rows, lanes] - 0.5625 * (e(j) + e(j + 1)) + 0.0625 * (e(j - 1) + e(j + 2))

                    def smooth(d, j):
                        put(2 * j, e(j) + 0.28125 * (d[j - 1] + d[j]) - 0.03125 * (d[j - 2] + d[j + 1]))

                    if not edges:
                        d = {}
                        for j in range(1, half - 2):
                            d[j] = detail(j)
                            put(2 * j + 1, d[j])
                            if j >= 4:
                                smooth(d, j - 1)
                    else:
                        d = {j: out_ref[2 * j + 1, rows, lanes] for j in (1, 2, 3)}
                        d |= {j: detail(j) for j in (-2, -1, 0)}
                        put(1, d[0])
                        for j in (0, 1, 2):
                            smooth(d, j)
                        d = {j: out_ref[2 * j + 1, rows, lanes] for j in range(half - 5, half - 2)}
                        d |= {j: detail(j) for j in range(half - 2, half + 1)}
                        for j in (half - 2, half - 1):
                            put(2 * j + 1, d[j])
                        for j in range(half - 3, half):
                            smooth(d, j)
                return tuple(sums)

            mine = slice(z * n_lev, (z + 1) * n_lev)
            totals[mine] = lax.fori_loop(first, last, tile, tuple(totals[mine]))
        return totals

    tiles = ny // TILE
    totals = [jnp.zeros((TILE, LANES), F32) for _ in range(zb * n_lev)]
    with jax.named_scope("xin"):
        totals = x_stage(totals, False, 1, tiles - 1)
    relay(2)
    with jax.named_scope("wait_inner"):
        for copy in inner:
            copy.wait_recv()
    with jax.named_scope("xinner"):
        totals = x_stage(totals, True, 1, tiles - 1)
    for g in order:
        with jax.named_scope("wait_u"):
            for copy in near[g]:
                copy.wait_recv()
        with jax.named_scope("u"):
            at = pl.ds(g * grp, grp)
            more = dot_pair(wu_ref[...], u[:, at, :].reshape(6 * grp, nz))
            more = more.reshape(grp, 2 * TILE, nz)
            for k, rows in enumerate(outer_rows):
                q[at, rows, :] += more[:, k * TILE : (k + 1) * TILE, :]
    for k in range(3, len(hops)):
        relay(k)
    with jax.named_scope("xin2"):
        for t in (0, tiles - 1):
            totals = x_stage(totals, False, t, t + 1)
    for k, t in enumerate((0, tiles - 1)):
        with jax.named_scope("wait_outer"):
            for copy in outer[k]:
                copy.wait_recv()
        with jax.named_scope("xouter"):
            totals = x_stage(totals, True, t, t + 1)
    with jax.named_scope("line"):
        lane = lax.broadcasted_iota(jnp.int32, (1, LANES), 1)
        line = jnp.zeros((1, LANES), F32)
        cells = nx * ny * width
        for z in range(zb):
            for n in range(n_lev):
                mass = jnp.sum(totals[z * n_lev + n], keepdims=True) / cells
                line += jnp.where(lane == n * GROUPS + map_ref[0, 0, z], mass, 0.0)
        part[...] = line
        slots[me] = line

    def spread(r, c, t):
        return pltpu.make_async_remote_copy(
            src_ref=part, dst_ref=slots.at[me], send_sem=g_send.at[t],
            recv_sem=g_recv.at[me], device_id=(r, c), device_id_type=MESH,
        )

    def gather(r, c, t):
        return pltpu.make_async_remote_copy(
            src_ref=part, dst_ref=slots.at[t], send_sem=g_send.at[t],
            recv_sem=g_recv.at[t], device_id=(r, c), device_id_type=MESH,
        )

    def peers(visit):
        if devices <= UNROLL:
            for j in reversed(range(n_row)):
                for k in range(n_col):
                    if j or k:
                        r, c = away_r(j), away_c(k)
                        visit(r, c, r * n_col + c)
            return

        @pl.loop(1, n_row)
        def _(j):
            @pl.loop(0, n_col)
            def _(k):
                r, c = lax.rem(row + j, n_row), lax.rem(col + k, n_col)
                visit(r, c, r * n_col + c)

        @pl.loop(1, n_col)
        def _(k):
            c = lax.rem(col + k, n_col)
            visit(row, c, row * n_col + c)

    with jax.named_scope("spread"):
        peers(lambda r, c, t: spread(r, c, t).start())
    with jax.named_scope("wsend"):
        for copy in sends:
            copy.wait_send()
    with jax.named_scope("gather"):
        peers(lambda r, c, t: gather(r, c, t).wait())
    with jax.named_scope("sum"):
        total = jnp.sum(slots[...], axis=0)
        mass_ref[...] = jnp.concatenate(
            [total[:, n * GROUPS : (n + 1) * GROUPS] for n in range(n_lev)], 0
        )


def deliver(c_ref, m_ref, out_hbm, mass_hbm, sems, m_sem):
    count = sems.shape[0]
    size = c_ref.shape[0] // count
    copies = [pltpu.make_async_copy(m_ref, mass_hbm, m_sem)]
    for i in range(count):
        at = pl.ds(i * size, size)
        copies.append(pltpu.make_async_copy(c_ref.at[at], out_hbm.at[at], sems.at[i]))
    for copy in copies:
        copy.start()
    for copy in copies:
        copy.wait()


def solution(mesh):
    n_row, n_col = mesh.shape["row"], mesh.shape["col"]

    def shards(pressure, cut_exponent, group_map):
        nx, ny, nz = pressure.shape
        grp = 8
        devices = n_row * n_col
        local = local_matrix(ny)
        own, beyond = local[:, :ny], local[:, ny:]
        eye = np.eye(ny)
        take = lambda i: eye[i]
        near = np.stack(partials_low(take, ny) + partials_high(take))
        ws = np.einsum("ky,xw->kxwy", near, np.eye(grp)).reshape(6 * grp, grp * ny)
        wy = np.concatenate([np.kron(np.eye(grp), own), ws])
        rim = np.r_[0:TILE, ny - TILE : ny]
        spread = lambda planes: np.einsum("wp,yk->pykw", planes, beyond[rim]).reshape(
            planes.shape[1] * 2 * TILE, -1
        )
        wx, wc, wu = np.kron(np.eye(3), own), spread(np.eye(TILE, 6)), spread(np.eye(grp))
        twice = lambda w: np.tile(w, 2)
        weights = [jnp.asarray(w, BF16) for w in (twice(wx), wy, twice(wc), twice(wu))]
        vmem = pl.BlockSpec(memory_space=pltpu.VMEM)
        hbm = pl.BlockSpec(memory_space=pltpu.HBM)
        hops = len(doublings(n_row, n_col))
        n_sends = 8 + 2 * (nx // grp)
        found = pl.pallas_call(
            functools.partial(kernel, n_row, n_col, grp),
            out_shape=(
                pltpu.VMEM((nx, ny, nz), F32),
                pltpu.VMEM((len(LEVELS), GROUPS), F32),
            ),
            in_specs=[hbm] * (3 + len(weights)),
            out_specs=(vmem, vmem),
            scratch_shapes=[
                pltpu.VMEM((nx, ny, nz), F32),
                pltpu.VMEM((nx + 6, ny, nz), F32),
                pltpu.VMEM((6, ny, nz), F32),
                pltpu.VMEM((6, ny, nz), F32),
                pltpu.VMEM((6, TILE, nz), F32),
                pltpu.VMEM((6, TILE, nz), F32),
                pltpu.VMEM((6, nx, nz), F32),
                pltpu.VMEM((6, nx, nz), F32),
                pltpu.VMEM((1, LANES), F32),
                pltpu.VMEM((devices, 1, LANES), F32),
                pltpu.SMEM(cut_exponent.shape, jnp.int32),
                pltpu.SMEM(group_map.shape, jnp.int32),
                pltpu.VMEM((nz, nz), BF16),
                *(pltpu.VMEM(w.shape, BF16) for w in weights),
                pltpu.SemaphoreType.DMA((14,)),
                pltpu.SemaphoreType.DMA((len(weights) + 2,)),
                pltpu.SemaphoreType.DMA((n_sends,)),
                pltpu.SemaphoreType.DMA((n_sends,)),
                pltpu.SemaphoreType.DMA((devices,)),
                pltpu.SemaphoreType.DMA((devices,)),
                pltpu.SemaphoreType.REGULAR((max(hops, 1),)),
            ],
            compiler_params=pltpu.CompilerParams(
                collective_id=0, has_side_effects=True, vmem_limit_bytes=24 * 2**20
            ),
        )(*(pltpu.with_memory_space_constraint(x, pltpu.HBM) for x in (cut_exponent, group_map, pressure, *weights)))
        coeffs, mass = pl.pallas_call(
            deliver,
            out_shape=tuple(pltpu.HBM(f.shape, F32) for f in found),
            in_specs=[vmem] * 2,
            out_specs=(hbm, hbm),
            scratch_shapes=[pltpu.SemaphoreType.DMA((8,)), pltpu.SemaphoreType.DMA],
            compiler_params=pltpu.CompilerParams(vmem_limit_bytes=2**20),
        )(*(pltpu.with_memory_space_constraint(x, pltpu.VMEM) for x in found))
        return coeffs, mass.T

    specs = P("row", "col", None)
    return jax.shard_map(
        shards, mesh=mesh, in_specs=(specs,) * 3, out_specs=(specs, P()), check_vma=False
    )
```

```python
import functools

import jax
import jax.numpy as jnp
import numpy as np
from jax import lax
from jax.experimental import pallas as pl
from jax.experimental.pallas import tpu as pltpu
from jax.sharding import PartitionSpec as P

GROUPS = 16
LEVELS = (0.25, 0.5, 1.0, 2.0)
MESH = pl.DeviceIdType.MESH
F32, BF16 = jnp.float32, jnp.bfloat16
TILE, LANES = 8, 128
UNROLL = 64


def cyclic_matrix(n):
    ev, od = np.eye(n)[0::2], np.eye(n)[1::2]
    r = lambda a, k: np.roll(a, k, 0)
    d = od - (0.5625 * (ev + r(ev, -1)) - 0.0625 * (r(ev, 1) + r(ev, -2)))
    s = ev + (0.28125 * (r(d, 1) + d) - 0.03125 * (r(d, 2) + r(d, -1)))
    return np.stack([s, d], 1).reshape(n, n)


def local_matrix(n):
    half = n // 2
    t = np.eye(n + 6)
    v, (a, b, c, f0, f1, g) = t[:n], t[n:]
    e = {j: v[2 * j] for j in range(half)}
    o = {j: v[2 * j + 1] for j in range(half)}
    e[-1], e[half], e[half + 1] = a, f0, f1
    d = {
        j: o[j] - 0.5625 * (e[j] + e[j + 1]) + 0.0625 * (e[j - 1] + e[j + 2])
        for j in range(half)
    }
    d[-1] = b - 0.5625 * e[0] + 0.0625 * e[1]
    d[-2] = c + 0.0625 * e[0]
    d[half] = g + 0.0625 * e[half - 1]
    out = np.zeros((n, n + 6))
    for j in range(half):
        out[2 * j] = e[j] + 0.28125 * (d[j - 1] + d[j]) - 0.03125 * (d[j - 2] + d[j + 1])
        out[2 * j + 1] = d[j]
    return out


def partials_low(row, n):
    a = row(n - 2)
    b = row(n - 1) - 0.5625 * a + 0.0625 * row(n - 4)
    c = row(n - 3) - 0.5625 * (row(n - 4) + a) + 0.0625 * row(n - 6)
    return a, b, c


def partials_high(row):
    f0, f1 = row(0), row(2)
    return f0, f1, row(1) - 0.5625 * (f0 + f1) + 0.0625 * row(4)


def split(value):
    hi = value.astype(BF16)
    return hi, (value - hi.astype(F32)).astype(BF16)


def dot2(left, right):
    dot = functools.partial(jnp.dot, preferred_element_type=F32)
    if left.dtype == BF16:
        hi, lo = split(right)
        return dot(left, hi) + dot(left, lo)
    hi, lo = split(left)
    return dot(hi, right) + dot(lo, right)


def dot_pair(left, right):
    return jnp.dot(left, jnp.concatenate(split(right), 0), preferred_element_type=F32)


def doublings(n_row, n_col):
    hops, known = [], 1
    while known < n_col // 2:
        hops.append((1, known))
        known *= 2
    known = 0
    while known < n_row // 2:
        hops.append((0, max(known, 1)))
        known += max(known, 1)
    return hops


def band(first_row, coefs):
    shape = (2 * TILE, LANES)
    lane = lax.broadcasted_iota(jnp.int32, shape, 1)
    far = jnp.abs(lane - lax.broadcasted_iota(jnp.int32, shape, 0) + first_row)
    value = jnp.zeros(shape, F32)
    for k, (even, odd) in enumerate(coefs):
        if even or odd:
            value = jnp.where(far == k, jnp.where(lane % 2 == 1, odd, even), value)
    return value.astype(BF16)


def fill_cyclic(ref):
    n = ref.shape[0]
    full = cyclic_matrix(n)
    reach = 7
    coefs = [(float(full[0, k]), float(full[1, 1 + k])) for k in range(reach)]
    made = {}
    for r in range(0, n, 2 * TILE):
        for c in range(0, n, LANES):
            off = (c - r + n // 2) % n - n // 2
            near = off - 2 * TILE < reach and off + LANES > -reach
            key = off if near else None
            if key not in made:
                made[key] = band(off, coefs) if near else jnp.zeros((2 * TILE, LANES), BF16)
            ref[pl.ds(r, 2 * TILE), pl.ds(c, LANES)] = made[key]


def kernel(n_row, n_col, grp, cut_hbm, map_hbm, p_ref, *refs):
    weights, refs = refs[:4], refs[4:]
    out_ref, mass_ref = refs[:2]
    ext, q, hs, yh, sh, ch, su, u, part, slots, cut_ref, map_ref, wz_ref = refs[2:15]
    held = refs[15:19]
    wx_ref, wy_ref, wc_ref, wu_ref = held
    in_sem, w_sem, h_send, h_recv, g_send, g_recv, hop_sem, last_sem = refs[19:]
    nx, ny, nz = p_ref.shape
    half = nx // 2
    devices = n_row * n_col
    row, col = lax.axis_index("row"), lax.axis_index("col")
    me = row * n_col + col
    away_r = lambda k: lax.rem(row + (k + n_row), n_row)
    away_c = lambda k: lax.rem(col + (k + n_col), n_col)
    up_r, dn_r, up_c, dn_c = away_r(1), away_r(-1), away_c(1), away_c(-1)

    barrier = pltpu.get_barrier_semaphore()
    top = n_row - 1
    at_first, at_last = row == 0, row == top

    def signal(sem, r, c):
        pl.semaphore_signal(sem, inc=1, device_id=(r, c), device_id_type=MESH)

    for r, c in ((dn_r, col), (row, up_c), (row, dn_c)):
        signal(barrier, r, c)
    pl.when(jnp.logical_not(at_last))(lambda: signal(barrier, row + 1, col))

    fetched = [
        pltpu.make_async_copy(src, dst, w_sem.at[i])
        for i, (src, dst) in enumerate(
            zip((*weights, cut_hbm, map_hbm), (*held, cut_ref, map_ref), strict=True)
        )
    ]
    odd_core = lax.rem(col, 2)

    def first_way(r):
        return lax.select(r == 0, 0, lax.select(r == top, odd_core, 1 - odd_core))

    ways = (first_way(row), 1 - first_way(row))
    needs = ((nx - 2, nx - 1, nx - 4, nx - 3, nx - 6), (0, 2, 1, 4))
    rest = sorted(set(range(nx)) - set(sum(needs, ())))

    def planes_of(way, act):
        for k, plane in enumerate(needs[way]):
            at = pl.ds(plane, 1)
            act(pltpu.make_async_copy(p_ref.at[at], ext.at[at], in_sem.at[5 * way + k]))

    for flip in range(2):
        for way in range(2):
            pl.when(ways[flip] == way)(lambda: planes_of(way, lambda copy: copy.start()))
    fetched[0].start()

    hops = doublings(n_row, n_col)

    def call(k):
        axis, far = hops[k]
        if axis:
            aim = ((row, away_c(far)), (row, away_c(-far)))
        else:
            aim = ((away_r(far), col), (away_r(-far), col))
        for to in aim:
            signal(hop_sem.at[k], *to)

    def relay(k):
        if k < len(hops):
            with jax.named_scope(f"r{k}"):
                pl.semaphore_wait(hop_sem.at[k], 2)
                if k + 1 < len(hops):
                    call(k + 1)

    sends = []

    def remote(i, src, dst, to):
        return pltpu.make_async_remote_copy(
            src_ref=src, dst_ref=dst, send_sem=h_send.at[i], recv_sem=h_recv.at[i],
            device_id=to, device_id_type=MESH,
        )

    def send(src, dst, to):
        copy = remote(len(sends), src, dst, to)
        copy.start()
        sends.append(copy)
        return copy

    def halo(piece, way):
        if isinstance(piece, int) and piece == 0:
            rows = pl.ds(TILE, ny - 2 * TILE)
        else:
            rows = pl.ds(pl.multiple_of((piece - 1) * (ny - TILE), TILE), TILE)
        three = lambda at: pl.ds(at + 3 * way, 3)
        to = lax.rem(row + 1 + way * (n_row - 2), n_row)
        return remote(
            2 + 2 * piece + way, yh.at[three(0), rows], q.at[three(nx), rows], (to, col)
        )

    with jax.named_scope("wz"):
        fill_cyclic(wz_ref)
        sh[:, pl.ds(6, TILE - 6), :] = jnp.zeros((6, TILE - 6, nz), F32)
    def call_first():
        pl.semaphore_wait(barrier, 4)
        signal(last_sem, 0, col)

    with jax.named_scope("barl"):
        pl.when(at_last)(call_first)

    def prepare(way):
        planes_of(way, lambda copy: copy.wait())
        made = (partials_low, partials_high)[way]
        planes = made(lambda i: ext[i], *((nx,) if way == 0 else ()))
        for i, plane in enumerate(planes):
            hs[3 * way + i] = plane

    with jax.named_scope("hs0"):
        for way in range(2):
            pl.when(ways[0] == way)(lambda: prepare(way))
        fetched[0].wait()
    inside = 3 * (ny - 2 * TILE)
    inner_rows = pl.ds(TILE, ny - 2 * TILE)
    outer_rows = (pl.ds(0, TILE), pl.ds(ny - TILE, TILE))
    plane_rows = lambda way: hs[pl.ds(3 * way, 3)].reshape(3 * ny, nz)

    def lift_inner(way, data):
        made = dot_pair(wx_ref[pl.ds(0, inside)], data)
        yh[pl.ds(3 * way, 3), inner_rows, :] = made.reshape(3, ny - 2 * TILE, nz)

    def lift_outer(way, data):
        made = dot_pair(wx_ref[pl.ds(inside, 6 * TILE)], data).reshape(3, 2 * TILE, nz)
        for k, rows in enumerate(outer_rows):
            yh[pl.ds(3 * way, 3), rows, :] = made[:, k * TILE : (k + 1) * TILE, :]

    with jax.named_scope("lift0"):
        lift_inner(ways[0], plane_rows(ways[0]))
    with jax.named_scope("bar"):
        pl.when(at_first)(lambda: pl.semaphore_wait(barrier, 3))
        pl.when(jnp.logical_not(at_first | at_last))(lambda: pl.semaphore_wait(barrier, 4))
    halo(0, ways[0]).start()
    with jax.named_scope("hs1"):
        for way in range(2):
            pl.when(ways[1] == way)(lambda: prepare(way))
        for i in range(6):
            line = lambda j: hs[i, pl.ds(j, 1), :]
            for k, one in enumerate(partials_low(line, ny) + partials_high(line)):
                sh[k, pl.ds(i, 1), :] = one
    lo, hi = pl.ds(0, 3), pl.ds(3, 3)
    corner = [
        send(sh.at[lo], ch.at[lo], (row, up_c)),
        send(sh.at[hi], ch.at[hi], (row, dn_c)),
    ]
    inner, *outer = [[halo(piece, way) for way in range(2)] for piece in range(3)]
    sends.extend(inner + outer[0] + outer[1])
    if hops:
        call(0)
    loads = []
    for i in range(3):
        at = pl.ds(5 + i * ((nx - 11) // 3), (nx - 11) // 3)
        if i == 2:
            at = pl.ds(5 + 2 * ((nx - 11) // 3), nx - 11 - 2 * ((nx - 11) // 3))
        loads.append(pltpu.make_async_copy(p_ref.at[at], ext.at[at], in_sem.at[10 + i]))
    for i, plane in enumerate((3, nx - 5)):
        at = pl.ds(plane, 1)
        loads.append(pltpu.make_async_copy(p_ref.at[at], ext.at[at], in_sem.at[13 + i]))
    for copy in loads:
        copy.start()
    for fetch in fetched[1:]:
        fetch.start()
    with jax.named_scope("lift1"):
        lifted = dot2(plane_rows(ways[1]), wz_ref[...])
        lift_inner(ways[1], lifted)
    pl.when(jnp.logical_not(at_first))(lambda: halo(0, ways[1]).start())
    with jax.named_scope("lift2"):
        lift_outer(ways[1], lifted)
        lift_outer(ways[0], dot2(plane_rows(ways[0]), wz_ref[...]))

    far = lax.select(at_first, 1, lax.select(at_last, 0, odd_core))
    tail = (
        (1, far + odd_core - 2 * far * odd_core), (2 - odd_core, far),
        (1 + odd_core, odd_core * far + (1 - odd_core) * (1 - far)), (2, 1 - far),
    )
    groups = nx // grp
    near = {}

    def z_group(g):
        at = pl.ds(g * grp, grp)
        v = dot2(ext[at].reshape(grp * ny, nz), wz_ref[...])
        got = dot2(wy_ref[...], v)
        q[at] = got[: grp * ny].reshape(grp, ny, nz)
        su[:, at, :] = got[grp * ny :].reshape(6, grp, nz)
        near[g] = (
            send(su.at[lo, at], u.at[lo, at], (row, up_c)),
            send(su.at[hi, at], u.at[hi, at], (row, dn_c)),
        )

    with jax.named_scope("ld2"):
        for copy in loads:
            copy.wait()
        for fetch in fetched[1:]:
            fetch.wait()
    order = (0, groups - 1, *range(1, groups - 1))
    with jax.named_scope("z"):
        for g in order[: groups // 2]:
            z_group(g)
    with jax.named_scope("last"):

        @pl.when(at_first)
        def _():
            pl.semaphore_wait(last_sem, 1)
            halo(0, ways[1]).start()

    relay(0)
    with jax.named_scope("z2"):
        z_group(order[groups // 2])
    with jax.named_scope("wait_corner"):
        for copy in corner:
            copy.wait_recv()
    with jax.named_scope("outer"):
        lifted = dot2(ch[...].reshape(6 * TILE, nz), wz_ref[...])
        more = dot_pair(wc_ref[...], lifted).reshape(6, 2 * TILE, nz)
        for k, rows in enumerate(outer_rows):
            yh[:, rows, :] += more[:, k * TILE : (k + 1) * TILE, :]
        for piece, way in tail:
            halo(piece, way).start()
    with jax.named_scope("z3"):
        for g in order[groups // 2 + 1 :]:
            z_group(g)
    relay(1)

    zb = cut_ref.shape[2]
    width = nz // zb
    n_lev = len(LEVELS)
    odd = lambda axis: lax.broadcasted_iota(jnp.int32, (TILE, LANES), axis) % 2
    mixed = (odd(0) + odd(1)) > 0

    def x_stage(totals, edges, first, last):
        totals = list(totals)
        for z in range(zb):
            cuts = jnp.full((TILE, LANES), -cut_ref[0, 0, z], jnp.int32)
            scale = jnp.exp2(cuts.astype(F32))
            limits = [level * scale for level in LEVELS]

            def tile(t, sums, z=z, limits=limits):
                rows = pl.ds(pl.multiple_of(t * TILE, TILE), TILE)
                sums = list(sums)
                for at in range(z * width, (z + 1) * width, LANES):
                    lanes = pl.ds(at, LANES)

                    def put(plane, value):
                        out_ref[plane, rows, lanes] = value
                        size = jnp.abs(value)
                        if plane % 2 == 0:
                            size = jnp.where(mixed, size, 0.0)
                        for n, limit in enumerate(limits):
                            sums[n] += jnp.maximum(size - limit, 0.0)

                    far = {-1: nx, half: nx + 3, half + 1: nx + 4}
                    e = lambda j: q[far.get(j, 2 * j), rows, lanes]

                    def detail(j):
                        if j == -1:
                            return q[nx + 1, rows, lanes] - 0.5625 * e(0) + 0.0625 * e(1)
                        if j == -2:
                            return q[nx + 2, rows, lanes] + 0.0625 * e(0)
                        if j == half:
                            return q[nx + 5, rows, lanes] + 0.0625 * e(half - 1)
                        return q[2 * j + 1, rows, lanes] - 0.5625 * (e(j) + e(j + 1)) + 0.0625 * (e(j - 1) + e(j + 2))

                    def smooth(d, j):
                        put(2 * j, e(j) + 0.28125 * (d[j - 1] + d[j]) - 0.03125 * (d[j - 2] + d[j + 1]))

                    if not edges:
                        d = {}
                        for j in range(1, half - 2):
                            d[j] = detail(j)
                            put(2 * j + 1, d[j])
                            if j >= 4:
                                smooth(d, j - 1)
                    else:
                        d = {j: out_ref[2 * j + 1, rows, lanes] for j in (1, 2, 3)}
                        d |= {j: detail(j) for j in (-2, -1, 0)}
                        put(1, d[0])
                        for j in (0, 1, 2):
                            smooth(d, j)
                        d = {j: out_ref[2 * j + 1, rows, lanes] for j in range(half - 5, half - 2)}
                        d |= {j: detail(j) for j in range(half - 2, half + 1)}
                        for j in (half - 2, half - 1):
                            put(2 * j + 1, d[j])
                        for j in range(half - 3, half):
                            smooth(d, j)
                return tuple(sums)

            mine = slice(z * n_lev, (z + 1) * n_lev)
            totals[mine] = lax.fori_loop(first, last, tile, tuple(totals[mine]))
        return totals

    tiles = ny // TILE
    totals = [jnp.zeros((TILE, LANES), F32) for _ in range(zb * n_lev)]
    with jax.named_scope("xin"):
        totals = x_stage(totals, False, 1, tiles - 1)
    relay(2)
    with jax.named_scope("wait_inner"):
        for copy in inner:
            copy.wait_recv()

        def make_up(way):
            at = pl.ds(nx + 3 * way, 3)
            raw = q[at, inner_rows, :].reshape(inside, nz)
            q[at, inner_rows, :] = dot2(raw, wz_ref[...]).reshape(3, ny - 2 * TILE, nz)

        pl.when(first_way(dn_r) == 0)(lambda: make_up(0))
        pl.when(first_way(up_r) == 1)(lambda: make_up(1))
    with jax.named_scope("xinner"):
        totals = x_stage(totals, True, 1, tiles - 1)
    for g in order:
        with jax.named_scope("wait_u"):
            for copy in near[g]:
                copy.wait_recv()
        with jax.named_scope("u"):
            at = pl.ds(g * grp, grp)
            more = dot_pair(wu_ref[...], u[:, at, :].reshape(6 * grp, nz))
            more = more.reshape(grp, 2 * TILE, nz)
            for k, rows in enumerate(outer_rows):
                q[at, rows, :] += more[:, k * TILE : (k + 1) * TILE, :]
    for k in range(3, len(hops)):
        relay(k)
    with jax.named_scope("xin2"):
        for t in (0, tiles - 1):
            totals = x_stage(totals, False, t, t + 1)
    for k, t in enumerate((0, tiles - 1)):
        with jax.named_scope("wait_outer"):
            for copy in outer[k]:
                copy.wait_recv()
        with jax.named_scope("xouter"):
            totals = x_stage(totals, True, t, t + 1)
    with jax.named_scope("line"):
        rows = zb * n_lev
        lane, at = (lax.broadcasted_iota(jnp.int32, (rows, LANES), axis) for axis in (1, 0))
        group = jnp.full((rows, LANES), map_ref[0, 0, 0], jnp.int32)
        for z in range(1, zb):
            group = jnp.where(at >= z * n_lev, map_ref[0, 0, z], group)
        sums = jnp.concatenate([jnp.sum(total, axis=0, keepdims=True) for total in totals], 0)
        mass = jnp.sum(sums, axis=1, keepdims=True) / (nx * ny * width)
        line = jnp.where(lane == at % n_lev * GROUPS + group, mass, 0.0)
        line = jnp.sum(line, axis=0, keepdims=True)
        part[...] = line
        slots[me] = line

    def spread(r, c, t):
        return pltpu.make_async_remote_copy(
            src_ref=part, dst_ref=slots.at[me], send_sem=g_send.at[t],
            recv_sem=g_recv.at[me], device_id=(r, c), device_id_type=MESH,
        )

    def gather(r, c, t):
        return pltpu.make_async_remote_copy(
            src_ref=part, dst_ref=slots.at[t], send_sem=g_send.at[t],
            recv_sem=g_recv.at[t], device_id=(r, c), device_id_type=MESH,
        )

    def peers(visit):
        if devices <= UNROLL:
            for j in (*range(1, n_row), 0):
                for k in range(n_col):
                    if j or k:
                        r, c = away_r(j), away_c(k)
                        visit(r, c, r * n_col + c)
            return

        @pl.loop(1, n_row)
        def _(j):
            @pl.loop(0, n_col)
            def _(k):
                r, c = lax.rem(row + j, n_row), lax.rem(col + k, n_col)
                visit(r, c, r * n_col + c)

        @pl.loop(1, n_col)
        def _(k):
            c = lax.rem(col + k, n_col)
            visit(row, c, row * n_col + c)

    with jax.named_scope("spread"):
        peers(lambda r, c, t: spread(r, c, t).start())
    with jax.named_scope("wsend"):
        for copy in sends:
            copy.wait_send()
    with jax.named_scope("gather"):
        peers(lambda r, c, t: gather(r, c, t).wait())
    mass_ref[...] = slots[...]


def deliver(c_ref, m_ref, out_hbm, mass_hbm, mass, sems, m_sem):
    count = sems.shape[0]
    size = c_ref.shape[0] // count
    copies = []
    for i in range(count):
        at = pl.ds(i * size, size)
        copies.append(pltpu.make_async_copy(c_ref.at[at], out_hbm.at[at], sems.at[i]))
        copies[i].start()
    total = jnp.sum(m_ref[...], axis=0)
    mass[...] = jnp.concatenate(
        [total[:, n * GROUPS : (n + 1) * GROUPS] for n in range(len(LEVELS))], 0
    )
    copies.append(pltpu.make_async_copy(mass, mass_hbm, m_sem))
    copies[-1].start()
    for copy in copies:
        copy.wait()


def solution(mesh):
    n_row, n_col = mesh.shape["row"], mesh.shape["col"]

    def shards(pressure, cut_exponent, group_map):
        nx, ny, nz = pressure.shape
        grp = 8
        devices = n_row * n_col
        local = local_matrix(ny)
        own, beyond = local[:, :ny], local[:, ny:]
        eye = np.eye(ny)
        take = lambda i: eye[i]
        near = np.stack(partials_low(take, ny) + partials_high(take))
        ws = np.einsum("ky,xw->kxwy", near, np.eye(grp)).reshape(6 * grp, grp * ny)
        wy = np.concatenate([np.kron(np.eye(grp), own), ws])
        rim = np.r_[0:TILE, ny - TILE : ny]
        spread = lambda planes: np.einsum("wp,yk->pykw", planes, beyond[rim]).reshape(
            planes.shape[1] * 2 * TILE, -1
        )
        core = np.r_[TILE : ny - TILE]
        wx = np.concatenate([np.kron(np.eye(3), own[rows]) for rows in (core, rim)])
        wc, wu = spread(np.eye(TILE, 6)), spread(np.eye(grp))
        twice = lambda w: np.tile(w, 2)
        weights = [jnp.asarray(w, BF16) for w in (twice(wx), wy, twice(wc), twice(wu))]
        vmem = pl.BlockSpec(memory_space=pltpu.VMEM)
        hbm = pl.BlockSpec(memory_space=pltpu.HBM)
        hops = len(doublings(n_row, n_col))
        n_sends = 8 + 2 * (nx // grp)
        found = pl.pallas_call(
            functools.partial(kernel, n_row, n_col, grp),
            out_shape=(
                pltpu.VMEM((nx, ny, nz), F32),
                pltpu.VMEM((devices, 1, LANES), F32),
            ),
            in_specs=[hbm] * (3 + len(weights)),
            out_specs=(vmem, vmem),
            scratch_shapes=[
                pltpu.VMEM((nx, ny, nz), F32),
                pltpu.VMEM((nx + 6, ny, nz), F32),
                pltpu.VMEM((6, ny, nz), F32),
                pltpu.VMEM((6, ny, nz), F32),
                pltpu.VMEM((6, TILE, nz), F32),
                pltpu.VMEM((6, TILE, nz), F32),
                pltpu.VMEM((6, nx, nz), F32),
                pltpu.VMEM((6, nx, nz), F32),
                pltpu.VMEM((1, LANES), F32),
                pltpu.VMEM((devices, 1, LANES), F32),
                pltpu.SMEM(cut_exponent.shape, jnp.int32),
                pltpu.SMEM(group_map.shape, jnp.int32),
                pltpu.VMEM((nz, nz), BF16),
                *(pltpu.VMEM(w.shape, BF16) for w in weights),
                pltpu.SemaphoreType.DMA((15,)),
                pltpu.SemaphoreType.DMA((len(weights) + 2,)),
                pltpu.SemaphoreType.DMA((n_sends,)),
                pltpu.SemaphoreType.DMA((n_sends,)),
                pltpu.SemaphoreType.DMA((devices,)),
                pltpu.SemaphoreType.DMA((devices,)),
                pltpu.SemaphoreType.REGULAR((max(hops, 1),)),
                pltpu.SemaphoreType.REGULAR,
            ],
            compiler_params=pltpu.CompilerParams(
                collective_id=0, has_side_effects=True, vmem_limit_bytes=24 * 2**20
            ),
        )(*(pltpu.with_memory_space_constraint(x, pltpu.HBM) for x in (cut_exponent, group_map, pressure, *weights)))
        coeffs, mass = pl.pallas_call(
            deliver,
            out_shape=(
                pltpu.HBM((nx, ny, nz), F32), pltpu.HBM((len(LEVELS), GROUPS), F32),
            ),
            in_specs=[vmem] * 2,
            out_specs=(hbm, hbm),
            scratch_shapes=[
                pltpu.VMEM((len(LEVELS), GROUPS), F32),
                pltpu.SemaphoreType.DMA((2,)),
                pltpu.SemaphoreType.DMA,
            ],
            compiler_params=pltpu.CompilerParams(vmem_limit_bytes=2**20),
        )(*(pltpu.with_memory_space_constraint(x, pltpu.VMEM) for x in found))
        return coeffs, mass.T

    specs = P("row", "col", None)
    return jax.shard_map(
        shards, mesh=mesh, in_specs=(specs,) * 3, out_specs=(specs, P()), check_vma=False
    )
```

```python
import functools

import jax
import jax.numpy as jnp
import numpy as np
from jax import lax
from jax.experimental import pallas as pl
from jax.experimental.pallas import tpu as pltpu
from jax.sharding import PartitionSpec as P

GROUPS = 16
LEVELS = (0.25, 0.5, 1.0, 2.0)
MESH = pl.DeviceIdType.MESH
F32, BF16 = jnp.float32, jnp.bfloat16
TILE, LANES = 8, 128
UNROLL = 64


def cyclic_matrix(n):
    ev, od = np.eye(n)[0::2], np.eye(n)[1::2]
    r = lambda a, k: np.roll(a, k, 0)
    d = od - (0.5625 * (ev + r(ev, -1)) - 0.0625 * (r(ev, 1) + r(ev, -2)))
    s = ev + (0.28125 * (r(d, 1) + d) - 0.03125 * (r(d, 2) + r(d, -1)))
    return np.stack([s, d], 1).reshape(n, n)


def local_matrix(n):
    half = n // 2
    t = np.eye(n + 6)
    v, (a, b, c, f0, f1, g) = t[:n], t[n:]
    e = {j: v[2 * j] for j in range(half)}
    o = {j: v[2 * j + 1] for j in range(half)}
    e[-1], e[half], e[half + 1] = a, f0, f1
    d = {
        j: o[j] - 0.5625 * (e[j] + e[j + 1]) + 0.0625 * (e[j - 1] + e[j + 2])
        for j in range(half)
    }
    d[-1] = b - 0.5625 * e[0] + 0.0625 * e[1]
    d[-2] = c + 0.0625 * e[0]
    d[half] = g + 0.0625 * e[half - 1]
    out = np.zeros((n, n + 6))
    for j in range(half):
        out[2 * j] = e[j] + 0.28125 * (d[j - 1] + d[j]) - 0.03125 * (d[j - 2] + d[j + 1])
        out[2 * j + 1] = d[j]
    return out


def partials_low(row, n):
    a = row(n - 2)
    b = row(n - 1) - 0.5625 * a + 0.0625 * row(n - 4)
    c = row(n - 3) - 0.5625 * (row(n - 4) + a) + 0.0625 * row(n - 6)
    return a, b, c


def partials_high(row):
    f0, f1 = row(0), row(2)
    return f0, f1, row(1) - 0.5625 * (f0 + f1) + 0.0625 * row(4)


def split(value):
    hi = value.astype(BF16)
    return hi, (value - hi.astype(F32)).astype(BF16)


def dot2(left, right):
    dot = functools.partial(jnp.dot, preferred_element_type=F32)
    if left.dtype == BF16:
        hi, lo = split(right)
        return dot(left, hi) + dot(left, lo)
    hi, lo = split(left)
    return dot(hi, right) + dot(lo, right)


def dot_pair(left, right):
    return jnp.dot(left, jnp.concatenate(split(right), 0), preferred_element_type=F32)


def doublings(n_row, n_col):
    hops, known = [], 1
    while known < n_col // 2:
        hops.append((1, known))
        known *= 2
    known = 0
    while known < n_row // 2:
        hops.append((0, max(known, 1)))
        known += max(known, 1)
    return hops


def band(first_row, coefs):
    shape = (2 * TILE, LANES)
    lane = lax.broadcasted_iota(jnp.int32, shape, 1)
    far = jnp.abs(lane - lax.broadcasted_iota(jnp.int32, shape, 0) + first_row)
    value = jnp.zeros(shape, F32)
    for k, (even, odd) in enumerate(coefs):
        if even or odd:
            value = jnp.where(far == k, jnp.where(lane % 2 == 1, odd, even), value)
    return value.astype(BF16)


def inner_twice(n):
    shape = (n - 2 * TILE, 2 * n)
    row, cell = (lax.broadcasted_iota(jnp.int32, shape, axis) for axis in (0, 1))
    far = jnp.abs(cell % n - row - TILE)
    value = jnp.zeros(shape, F32)
    for k, (even, odd) in enumerate(coefficients(n)):
        value = jnp.where(far == k, jnp.where(row % 2 == 1, odd, even), value)
    return value.astype(BF16)


def coefficients(n):
    full = cyclic_matrix(n)
    return [(float(full[0, k]), float(full[1, 1 + k])) for k in range(7)]


def fill_cyclic(ref):
    n = ref.shape[0]
    coefs = coefficients(n)
    reach = len(coefs)
    made = {}
    for r in range(0, n, 2 * TILE):
        for c in range(0, n, LANES):
            off = (c - r + n // 2) % n - n // 2
            near = off - 2 * TILE < reach and off + LANES > -reach
            key = off if near else None
            if key not in made:
                made[key] = band(off, coefs) if near else jnp.zeros((2 * TILE, LANES), BF16)
            ref[pl.ds(r, 2 * TILE), pl.ds(c, LANES)] = made[key]


def kernel(n_row, n_col, grp, cut_hbm, map_hbm, p_ref, *refs):
    weights, refs = refs[:2], refs[2:]
    out_ref, mass_ref = refs[:2]
    ext, q, hs, yh, sh, ch, su, u, part, slots, cut_ref, map_ref, wz_ref = refs[2:15]
    held = refs[15:17]
    wx_ref, wall_ref = held
    in_sem, w_sem, h_send, h_recv, g_sem, hop_sem, last_sem = refs[17:]
    nx, ny, nz = p_ref.shape
    half = nx // 2
    tall = grp * ny + 6 * grp
    wy_ref = wall_ref.at[pl.ds(0, tall)]
    wc_ref = wall_ref.at[pl.ds(tall, 12 * TILE), pl.ds(0, 12 * TILE)]
    wu_ref = wall_ref.at[pl.ds(tall + 12 * TILE, 2 * TILE * grp), pl.ds(0, 12 * grp)]
    devices = n_row * n_col
    row, col = lax.axis_index("row"), lax.axis_index("col")
    me = row * n_col + col
    away_r = lambda k: lax.rem(row + (k + n_row), n_row)
    away_c = lambda k: lax.rem(col + (k + n_col), n_col)
    up_r, dn_r, up_c, dn_c = away_r(1), away_r(-1), away_c(1), away_c(-1)

    barrier = pltpu.get_barrier_semaphore()
    top = n_row - 1
    at_first, at_last = row == 0, row == top

    def signal(sem, r, c):
        pl.semaphore_signal(sem, inc=1, device_id=(r, c), device_id_type=MESH)

    fetched = [
        pltpu.make_async_copy(src, dst, w_sem.at[i])
        for i, (src, dst) in enumerate(
            zip((*weights, cut_hbm, map_hbm), (*held, cut_ref, map_ref), strict=True)
        )
    ]
    odd_core = lax.rem(col, 2)

    def first_way(r):
        return lax.select(r == 0, 0, lax.select(r == top, odd_core, 1 - odd_core))

    ways = (first_way(row), 1 - first_way(row))
    needs = ((nx - 2, nx - 1, nx - 4, nx - 3, nx - 6), (0, 2, 1, 4))

    def take(at, i):
        return pltpu.make_async_copy(p_ref.at[at], ext.at[at], in_sem.at[i])

    def landed(ref, sem):
        pltpu.make_async_copy(ref, ref, sem).wait()

    head = lax.select(ways[0] == 0, needs[0][0], needs[1][0])
    head_copy = take(pl.ds(head, 1), 0)
    head_copy.start()
    fetched[0].start()
    for flip in range(2):
        for way in range(2):

            @pl.when(ways[flip] == way)
            def _():
                for plane in needs[way][1 - flip :]:
                    take(pl.ds(plane, 1), 1 + flip).start()

    loads = []
    mid = nx - 11
    starts = (5, 5 + mid // 3, 5 + 2 * (mid // 3), nx - 6)
    for at, end in (*zip(starts[:-1], starts[1:], strict=True), (3, 4), (nx - 5, nx - 4)):
        loads.append(take(pl.ds(at, end - at), 3))
    for copy in loads:
        copy.start()
    for fetch in fetched[1:]:
        fetch.start()

    for r, c in ((dn_r, col), (row, up_c), (row, dn_c)):
        signal(barrier, r, c)
    pl.when(jnp.logical_not(at_last))(lambda: signal(barrier, row + 1, col))

    hops = doublings(n_row, n_col)

    def call(k):
        axis, far = hops[k]
        if axis:
            aim = ((row, away_c(far)), (row, away_c(-far)))
        else:
            aim = ((away_r(far), col), (away_r(-far), col))
        for to in aim:
            signal(hop_sem.at[k], *to)

    def relay(k):
        if k < len(hops):
            with jax.named_scope(f"r{k}"):
                pl.semaphore_wait(hop_sem.at[k], 2)
                if k + 1 < len(hops):
                    call(k + 1)

    def remote(i, j, src, dst, to):
        return pltpu.make_async_remote_copy(
            src_ref=src, dst_ref=dst, send_sem=h_send.at[i], recv_sem=h_recv.at[j],
            device_id=to, device_id_type=MESH,
        )

    def halo(piece, way):
        first, count = 0, 3
        if isinstance(piece, int) and piece in (0, 3):
            rows = pl.ds(TILE, ny - 2 * TILE)
            first, count = (1, 2) if piece else (0, 1)
            piece = 0
        else:
            rows = pl.ds(pl.multiple_of((piece - 1) * (ny - TILE), TILE), TILE)
        planes = lambda at: pl.ds(at + 3 * way + first, count)
        to = lax.rem(row + 1 + way * (n_row - 2), n_row)
        return remote(0, piece, yh.at[planes(0), rows], q.at[planes(nx), rows], (to, col))

    with jax.named_scope("wz"):
        alone = inner_twice(ny)
        fill_cyclic(wz_ref)
        sh[:, pl.ds(6, TILE - 6), :] = jnp.zeros((6, TILE - 6, nz), F32)
    def call_first():
        pl.semaphore_wait(barrier, 4)
        signal(last_sem, 0, col)

    with jax.named_scope("barl"):
        pl.when(at_last)(call_first)

    def prepare(way, flip):
        landed(ext.at[pl.ds(0, len(needs[way]) - 1 + flip)], in_sem.at[1 + flip])
        made = (partials_low, partials_high)[way]
        planes = made(lambda i: ext[i], *((nx,) if way == 0 else ()))
        for i, plane in enumerate(planes):
            hs[3 * way + i] = plane

    inside = ny - 2 * TILE
    inner_rows = pl.ds(TILE, inside)
    outer_rows = (pl.ds(0, TILE), pl.ds(ny - TILE, TILE))
    plane_rows = lambda way: hs[pl.ds(3 * way, 3)].reshape(3 * ny, nz)

    def lift_inner(way, data, first):
        count = 3 - first
        made = dot_pair(wx_ref[pl.ds(first * inside, count * inside)], data)
        yh[pl.ds(3 * way + first, count), inner_rows, :] = made.reshape(count, inside, nz)

    def lift_outer(way, data):
        made = dot_pair(wx_ref[pl.ds(3 * inside, 6 * TILE)], data).reshape(3, 2 * TILE, nz)
        for k, rows in enumerate(outer_rows):
            yh[pl.ds(3 * way, 3), rows, :] = made[:, k * TILE : (k + 1) * TILE, :]

    with jax.named_scope("hs0"):
        head_copy.wait()
    with jax.named_scope("lift0"):
        yh[3 * ways[0], inner_rows, :] = dot_pair(alone, ext[head])
    with jax.named_scope("bar"):
        pl.when(at_first)(lambda: pl.semaphore_wait(barrier, 3))
        pl.when(jnp.logical_not(at_first | at_last))(lambda: pl.semaphore_wait(barrier, 4))
    halo(0, ways[0]).start()
    with jax.named_scope("lift0b"):
        for way in range(2):
            pl.when(ways[0] == way)(lambda: prepare(way, 0))
        fetched[0].wait()
        lift_inner(ways[0], plane_rows(ways[0]), 1)
    halo(3, ways[0]).start()
    with jax.named_scope("hs1"):
        for way in range(2):
            pl.when(ways[1] == way)(lambda: prepare(way, 1))
        for i in range(6):
            line = lambda j: hs[i, pl.ds(j, 1), :]
            for k, one in enumerate(partials_low(line, ny) + partials_high(line)):
                sh[k, pl.ds(i, 1), :] = one
    lo, hi = pl.ds(0, 3), pl.ds(3, 3)
    for half_k, c in ((lo, up_c), (hi, dn_c)):
        remote(1, 3, sh.at[half_k], ch.at[half_k], (row, c)).start()
    if hops:
        call(0)
    with jax.named_scope("lift1"):
        lifted = dot2(plane_rows(ways[1]), wz_ref[...])
        lift_inner(ways[1], lifted, 0)

    def second():
        halo(0, ways[1]).start()
        halo(3, ways[1]).start()

    pl.when(jnp.logical_not(at_first))(second)

    far = lax.select(at_first, 1, lax.select(at_last, 0, odd_core))
    tail = (
        (1, far + odd_core - 2 * far * odd_core), (2 - odd_core, far),
        (1 + odd_core, odd_core * far + (1 - odd_core) * (1 - far)), (2, 1 - far),
    )
    groups = nx // grp

    def z_group(g):
        at = pl.ds(g * grp, grp)
        v = dot2(ext[at].reshape(grp * ny, nz), wz_ref[...])
        got = dot2(wy_ref[...], v)
        q[at] = got[: grp * ny].reshape(grp, ny, nz)
        su[:, at, :] = got[grp * ny :].reshape(6, grp, nz)
        for half_k, c in ((lo, up_c), (hi, dn_c)):
            remote(2, 4 + g, su.at[half_k, at], u.at[half_k, at], (row, c)).start()

    with jax.named_scope("ld2"):
        landed(ext.at[pl.ds(0, nx - len(sum(needs, ())))], in_sem.at[3])
        for fetch in fetched[1:]:
            fetch.wait()
    order = (0, groups - 1, *range(1, groups - 1))
    with jax.named_scope("z"):
        for g in order[: groups // 2]:
            z_group(g)
    with jax.named_scope("lift2"):
        lift_outer(ways[1], lifted)
        lift_outer(ways[0], dot2(plane_rows(ways[0]), wz_ref[...]))
    with jax.named_scope("last"):

        @pl.when(at_first)
        def _():
            pl.semaphore_wait(last_sem, 1)
            second()

    relay(0)
    with jax.named_scope("z2"):
        z_group(order[groups // 2])
    with jax.named_scope("wait_corner"):
        landed(ch, h_recv.at[3])
    with jax.named_scope("outer"):
        lifted = dot2(ch[...].reshape(6 * TILE, nz), wz_ref[...])
        more = dot_pair(wc_ref[...], lifted).reshape(6, 2 * TILE, nz)
        for k, rows in enumerate(outer_rows):
            yh[:, rows, :] += more[:, k * TILE : (k + 1) * TILE, :]
        for piece, way in tail:
            halo(piece, way).start()
    with jax.named_scope("z3"):
        for g in order[groups // 2 + 1 :]:
            z_group(g)
    relay(1)

    zb = cut_ref.shape[2]
    width = nz // zb
    n_lev = len(LEVELS)
    odd = lambda axis: lax.broadcasted_iota(jnp.int32, (TILE, LANES), axis) % 2
    mixed = (odd(0) + odd(1)) > 0

    def x_stage(totals, edges, first, last):
        totals = list(totals)
        for z in range(zb):
            cuts = jnp.full((TILE, LANES), -cut_ref[0, 0, z], jnp.int32)
            scale = jnp.exp2(cuts.astype(F32))
            limits = [level * scale for level in LEVELS]

            def tile(t, sums, z=z, limits=limits):
                rows = pl.ds(pl.multiple_of(t * TILE, TILE), TILE)
                sums = list(sums)
                for at in range(z * width, (z + 1) * width, LANES):
                    lanes = pl.ds(at, LANES)

                    def put(plane, value):
                        out_ref[plane, rows, lanes] = value
                        size = jnp.abs(value)
                        if plane % 2 == 0:
                            size = jnp.where(mixed, size, 0.0)
                        for n, limit in enumerate(limits):
                            sums[n] += jnp.maximum(size - limit, 0.0)

                    far = {-1: nx, half: nx + 3, half + 1: nx + 4}
                    e = lambda j: q[far.get(j, 2 * j), rows, lanes]

                    def detail(j):
                        if j == -1:
                            return q[nx + 1, rows, lanes] - 0.5625 * e(0) + 0.0625 * e(1)
                        if j == -2:
                            return q[nx + 2, rows, lanes] + 0.0625 * e(0)
                        if j == half:
                            return q[nx + 5, rows, lanes] + 0.0625 * e(half - 1)
                        return q[2 * j + 1, rows, lanes] - 0.5625 * (e(j) + e(j + 1)) + 0.0625 * (e(j - 1) + e(j + 2))

                    def smooth(d, j):
                        put(2 * j, e(j) + 0.28125 * (d[j - 1] + d[j]) - 0.03125 * (d[j - 2] + d[j + 1]))

                    if not edges:
                        d = {}
                        for j in range(1, half - 2):
                            d[j] = detail(j)
                            put(2 * j + 1, d[j])
                            if j >= 4:
                                smooth(d, j - 1)
                    else:
                        d = {j: out_ref[2 * j + 1, rows, lanes] for j in (1, 2, 3)}
                        d |= {j: detail(j) for j in (-2, -1, 0)}
                        put(1, d[0])
                        for j in (0, 1, 2):
                            smooth(d, j)
                        d = {j: out_ref[2 * j + 1, rows, lanes] for j in range(half - 5, half - 2)}
                        d |= {j: detail(j) for j in range(half - 2, half + 1)}
                        for j in (half - 2, half - 1):
                            put(2 * j + 1, d[j])
                        for j in range(half - 3, half):
                            smooth(d, j)
                return tuple(sums)

            mine = slice(z * n_lev, (z + 1) * n_lev)
            totals[mine] = lax.fori_loop(first, last, tile, tuple(totals[mine]))
        return totals

    tiles = ny // TILE
    totals = [jnp.zeros((TILE, LANES), F32) for _ in range(zb * n_lev)]
    with jax.named_scope("xin"):
        totals = x_stage(totals, False, 1, tiles - 1)
    relay(2)
    with jax.named_scope("wait_inner"):
        landed(q.at[pl.ds(nx, 6), inner_rows], h_recv.at[0])

        def make_up(way):
            at = pl.ds(nx + 3 * way, 3)
            raw = q[at, inner_rows, :].reshape(3 * inside, nz)
            q[at, inner_rows, :] = dot2(raw, wz_ref[...]).reshape(3, inside, nz)

        pl.when(first_way(dn_r) == 0)(lambda: make_up(0))
        pl.when(first_way(up_r) == 1)(lambda: make_up(1))
    with jax.named_scope("xinner"):
        totals = x_stage(totals, True, 1, tiles - 1)
    for g in order:
        with jax.named_scope("wait_u"):
            landed(u.at[:, pl.ds(g * grp, grp)], h_recv.at[4 + g])
        with jax.named_scope("u"):
            at = pl.ds(g * grp, grp)
            more = dot_pair(wu_ref[...], u[:, at, :].reshape(6 * grp, nz))
            more = more.reshape(grp, 2 * TILE, nz)
            for k, rows in enumerate(outer_rows):
                q[at, rows, :] += more[:, k * TILE : (k + 1) * TILE, :]
    for k in range(3, len(hops)):
        relay(k)
    with jax.named_scope("xin2"):
        for t in (0, tiles - 1):
            totals = x_stage(totals, False, t, t + 1)
    for k, t in enumerate((0, tiles - 1)):
        with jax.named_scope("wait_outer"):
            landed(q.at[pl.ds(nx, 6), outer_rows[k]], h_recv.at[1 + k])
        with jax.named_scope("xouter"):
            totals = x_stage(totals, True, t, t + 1)
    with jax.named_scope("line"):
        rows = zb * n_lev
        lane, at = (lax.broadcasted_iota(jnp.int32, (rows, LANES), axis) for axis in (1, 0))
        group = jnp.full((rows, LANES), map_ref[0, 0, 0], jnp.int32)
        for z in range(1, zb):
            group = jnp.where(at >= z * n_lev, map_ref[0, 0, z], group)
        sums = jnp.concatenate([jnp.sum(total, axis=0, keepdims=True) for total in totals], 0)
        mass = jnp.sum(sums, axis=1, keepdims=True) / (nx * ny * width)
        line = jnp.where(lane == at % n_lev * GROUPS + group, mass, 0.0)
        line = jnp.sum(line, axis=0, keepdims=True)
        part[...] = line
        slots[me] = line

    def spread(r, c):
        pltpu.make_async_remote_copy(
            src_ref=part, dst_ref=slots.at[me], send_sem=g_sem.at[0],
            recv_sem=g_sem.at[1], device_id=(r, c), device_id_type=MESH,
        ).start()

    def peers(visit):
        if devices <= UNROLL:
            for j in (*range(1, n_row), 0):
                for k in range(n_col):
                    if j or k:
                        visit(away_r(j), away_c(k))
            return

        @pl.loop(1, n_row)
        def _(j):
            @pl.loop(0, n_col)
            def _(k):
                visit(lax.rem(row + j, n_row), lax.rem(col + k, n_col))

        @pl.loop(1, n_col)
        def _(k):
            visit(row, lax.rem(col + k, n_col))

    with jax.named_scope("spread"):
        peers(spread)
    with jax.named_scope("wsend"):
        for i, sent in enumerate((yh, sh, su)):
            landed(sent, h_send.at[i])
    with jax.named_scope("gather"):
        for i in range(2):
            landed(slots.at[pl.ds(0, devices - 1)], g_sem.at[i])
    mass_ref[...] = slots[...]


def deliver(c_ref, m_ref, out_hbm, mass_hbm, mass, sems, m_sem):
    count = sems.shape[0]
    size = c_ref.shape[0] // count
    copies = []
    for i in range(count):
        at = pl.ds(i * size, size)
        copies.append(pltpu.make_async_copy(c_ref.at[at], out_hbm.at[at], sems.at[i]))
        copies[i].start()
    total = jnp.sum(m_ref[...], axis=0)
    mass[...] = jnp.concatenate(
        [total[:, n * GROUPS : (n + 1) * GROUPS] for n in range(len(LEVELS))], 0
    )
    copies.append(pltpu.make_async_copy(mass, mass_hbm, m_sem))
    copies[-1].start()
    for copy in copies:
        copy.wait()


def solution(mesh):
    n_row, n_col = mesh.shape["row"], mesh.shape["col"]

    def shards(pressure, cut_exponent, group_map):
        nx, ny, nz = pressure.shape
        grp = 8
        devices = n_row * n_col
        local = local_matrix(ny)
        own, beyond = local[:, :ny], local[:, ny:]
        eye = np.eye(ny)
        take = lambda i: eye[i]
        near = np.stack(partials_low(take, ny) + partials_high(take))
        ws = np.einsum("ky,xw->kxwy", near, np.eye(grp)).reshape(6 * grp, grp * ny)
        wy = np.concatenate([np.kron(np.eye(grp), own), ws])
        rim = np.r_[0:TILE, ny - TILE : ny]
        spread = lambda planes: np.einsum("wp,yk->pykw", planes, beyond[rim]).reshape(
            planes.shape[1] * 2 * TILE, -1
        )
        core = np.r_[TILE : ny - TILE]
        twice = lambda w: np.tile(w, 2)
        wx = np.concatenate([twice(np.kron(np.eye(3), own[rows])) for rows in (core, rim)])
        wc, wu = spread(np.eye(TILE, 6)), spread(np.eye(grp))
        wide = lambda w: np.pad(w, ((0, 0), (0, wy.shape[1] - w.shape[1])))
        wall = np.concatenate([wy, wide(twice(wc)), wide(twice(wu))])
        weights = [jnp.asarray(w, BF16) for w in (wx, wall)]
        vmem = pl.BlockSpec(memory_space=pltpu.VMEM)
        hbm = pl.BlockSpec(memory_space=pltpu.HBM)
        hops = len(doublings(n_row, n_col))
        found = pl.pallas_call(
            functools.partial(kernel, n_row, n_col, grp),
            out_shape=(
                pltpu.VMEM((nx, ny, nz), F32),
                pltpu.VMEM((devices, 1, LANES), F32),
            ),
            in_specs=[hbm] * (3 + len(weights)),
            out_specs=(vmem, vmem),
            scratch_shapes=[
                pltpu.VMEM((nx, ny, nz), F32),
                pltpu.VMEM((nx + 6, ny, nz), F32),
                pltpu.VMEM((6, ny, nz), F32),
                pltpu.VMEM((6, ny, nz), F32),
                pltpu.VMEM((6, TILE, nz), F32),
                pltpu.VMEM((6, TILE, nz), F32),
                pltpu.VMEM((6, nx, nz), F32),
                pltpu.VMEM((6, nx, nz), F32),
                pltpu.VMEM((1, LANES), F32),
                pltpu.VMEM((devices, 1, LANES), F32),
                pltpu.SMEM(cut_exponent.shape, jnp.int32),
                pltpu.SMEM(group_map.shape, jnp.int32),
                pltpu.VMEM((nz, nz), BF16),
                *(pltpu.VMEM(w.shape, BF16) for w in weights),
                pltpu.SemaphoreType.DMA((4,)),
                pltpu.SemaphoreType.DMA((len(weights) + 2,)),
                pltpu.SemaphoreType.DMA((3,)),
                pltpu.SemaphoreType.DMA((4 + nx // grp,)),
                pltpu.SemaphoreType.DMA((2,)),
                pltpu.SemaphoreType.REGULAR((max(hops, 1),)),
                pltpu.SemaphoreType.REGULAR,
            ],
            compiler_params=pltpu.CompilerParams(
                collective_id=0, has_side_effects=True, vmem_limit_bytes=24 * 2**20
            ),
        )(*(pltpu.with_memory_space_constraint(x, pltpu.HBM) for x in (cut_exponent, group_map, pressure, *weights)))
        coeffs, mass = pl.pallas_call(
            deliver,
            out_shape=(
                pltpu.HBM((nx, ny, nz), F32), pltpu.HBM((len(LEVELS), GROUPS), F32),
            ),
            in_specs=[vmem] * 2,
            out_specs=(hbm, hbm),
            scratch_shapes=[
                pltpu.VMEM((len(LEVELS), GROUPS), F32),
                pltpu.SemaphoreType.DMA((2,)),
                pltpu.SemaphoreType.DMA,
            ],
            compiler_params=pltpu.CompilerParams(vmem_limit_bytes=2**20),
        )(*(pltpu.with_memory_space_constraint(x, pltpu.VMEM) for x in found))
        return coeffs, mass.T

    specs = P("row", "col", None)
    return jax.shard_map(
        shards, mesh=mesh, in_specs=(specs,) * 3, out_specs=(specs, P()), check_vma=False
    )
```

```python
import functools

import jax
import jax.numpy as jnp
import numpy as np
from jax import lax
from jax.experimental import pallas as pl
from jax.experimental.pallas import tpu as pltpu
from jax.sharding import PartitionSpec as P

GROUPS = 16
LEVELS = (0.25, 0.5, 1.0, 2.0)
MESH = pl.DeviceIdType.MESH
F32, BF16 = jnp.float32, jnp.bfloat16
TILE, LANES = 8, 128
UNROLL = 64


def cyclic_matrix(n):
    ev, od = np.eye(n)[0::2], np.eye(n)[1::2]
    r = lambda a, k: np.roll(a, k, 0)
    d = od - (0.5625 * (ev + r(ev, -1)) - 0.0625 * (r(ev, 1) + r(ev, -2)))
    s = ev + (0.28125 * (r(d, 1) + d) - 0.03125 * (r(d, 2) + r(d, -1)))
    return np.stack([s, d], 1).reshape(n, n)


def local_matrix(n):
    half = n // 2
    t = np.eye(n + 6)
    v, (a, b, c, f0, f1, g) = t[:n], t[n:]
    e = {j: v[2 * j] for j in range(half)}
    o = {j: v[2 * j + 1] for j in range(half)}
    e[-1], e[half], e[half + 1] = a, f0, f1
    d = {
        j: o[j] - 0.5625 * (e[j] + e[j + 1]) + 0.0625 * (e[j - 1] + e[j + 2])
        for j in range(half)
    }
    d[-1] = b - 0.5625 * e[0] + 0.0625 * e[1]
    d[-2] = c + 0.0625 * e[0]
    d[half] = g + 0.0625 * e[half - 1]
    out = np.zeros((n, n + 6))
    for j in range(half):
        out[2 * j] = e[j] + 0.28125 * (d[j - 1] + d[j]) - 0.03125 * (d[j - 2] + d[j + 1])
        out[2 * j + 1] = d[j]
    return out


def partials_low(row, n):
    a = row(n - 2)
    b = row(n - 1) - 0.5625 * a + 0.0625 * row(n - 4)
    c = row(n - 3) - 0.5625 * (row(n - 4) + a) + 0.0625 * row(n - 6)
    return a, b, c


def partials_high(row):
    f0, f1 = row(0), row(2)
    return f0, f1, row(1) - 0.5625 * (f0 + f1) + 0.0625 * row(4)


def split(value):
    hi = value.astype(BF16)
    return hi, (value - hi.astype(F32)).astype(BF16)


def dot2(left, right):
    dot = functools.partial(jnp.dot, preferred_element_type=F32)
    if left.dtype == BF16:
        hi, lo = split(right)
        return dot(left, hi) + dot(left, lo)
    hi, lo = split(left)
    return dot(hi, right) + dot(lo, right)


def dot_pair(left, right):
    return jnp.dot(left, jnp.concatenate(split(right), 0), preferred_element_type=F32)


def doublings(n_row, n_col):
    hops, known = [], 1
    while known < n_col // 2:
        hops.append((1, known))
        known *= 2
    known = 0
    while known < n_row // 2:
        hops.append((0, max(known, 1)))
        known += max(known, 1)
    return hops


def band(first_row, coefs):
    shape = (2 * TILE, LANES)
    lane = lax.broadcasted_iota(jnp.int32, shape, 1)
    far = jnp.abs(lane - lax.broadcasted_iota(jnp.int32, shape, 0) + first_row)
    value = jnp.zeros(shape, F32)
    for k, (even, odd) in enumerate(coefs):
        if even or odd:
            value = jnp.where(far == k, jnp.where(lane % 2 == 1, odd, even), value)
    return value.astype(BF16)


def inner_twice(n):
    shape = (n - 2 * TILE, 2 * n)
    row, cell = (lax.broadcasted_iota(jnp.int32, shape, axis) for axis in (0, 1))
    far = jnp.abs(cell % n - row - TILE)
    value = jnp.zeros(shape, F32)
    for k, (even, odd) in enumerate(coefficients(n)):
        value = jnp.where(far == k, jnp.where(row % 2 == 1, odd, even), value)
    return value.astype(BF16)


def coefficients(n):
    full = cyclic_matrix(n)
    return [(float(full[0, k]), float(full[1, 1 + k])) for k in range(7)]


def fill_cyclic(ref):
    n = ref.shape[0]
    coefs = coefficients(n)
    reach = len(coefs)
    made = {}
    for r in range(0, n, 2 * TILE):
        for c in range(0, n, LANES):
            off = (c - r + n // 2) % n - n // 2
            near = off - 2 * TILE < reach and off + LANES > -reach
            key = off if near else None
            if key not in made:
                made[key] = band(off, coefs) if near else jnp.zeros((2 * TILE, LANES), BF16)
            ref[pl.ds(r, 2 * TILE), pl.ds(c, LANES)] = made[key]


def kernel(n_row, n_col, grp, cut_hbm, map_hbm, p_ref, *refs):
    weights, refs = refs[:2], refs[2:]
    out_ref, mass_ref = refs[:2]
    ext, q, hs, yh, sh, ch, su, u, part, slots, cut_ref, map_ref, wz_ref = refs[2:15]
    held = refs[15:17]
    wx_ref, wall_ref = held
    in_sem, w_sem, h_send, h_recv, g_sem, hop_sem, last_sem = refs[17:]
    nx, ny, nz = p_ref.shape
    half = nx // 2
    tall = grp * ny + 6 * grp
    wy_ref = wall_ref.at[pl.ds(0, tall)]
    wc_ref = wall_ref.at[pl.ds(tall, 12 * TILE), pl.ds(0, 12 * TILE)]
    wu_ref = wall_ref.at[pl.ds(tall + 12 * TILE, 2 * TILE * grp), pl.ds(0, 12 * grp)]
    devices = n_row * n_col
    row, col = lax.axis_index("row"), lax.axis_index("col")
    me = row * n_col + col
    away_r = lambda k: lax.rem(row + (k + n_row), n_row)
    away_c = lambda k: lax.rem(col + (k + n_col), n_col)
    up_r, dn_r, up_c, dn_c = away_r(1), away_r(-1), away_c(1), away_c(-1)

    barrier = pltpu.get_barrier_semaphore()
    top = n_row - 1
    at_first, at_last = row == 0, row == top

    def signal(sem, r, c):
        pl.semaphore_signal(sem, inc=1, device_id=(r, c), device_id_type=MESH)

    for r, c in ((dn_r, col), (row, up_c), (row, dn_c)):
        signal(barrier, r, c)
    pl.when(jnp.logical_not(at_last))(lambda: signal(barrier, row + 1, col))

    fetched = [
        pltpu.make_async_copy(src, dst, w_sem.at[i])
        for i, (src, dst) in enumerate(
            zip((*weights, cut_hbm, map_hbm), (*held, cut_ref, map_ref), strict=True)
        )
    ]
    odd_core = lax.rem(col, 2)

    def first_way(r):
        return lax.select(r == 0, 0, lax.select(r == top, odd_core, 1 - odd_core))

    ways = (first_way(row), 1 - first_way(row))
    needs = ((nx - 2, nx - 1, nx - 4, nx - 3, nx - 6), (0, 2, 1, 4))

    def take(at, i):
        return pltpu.make_async_copy(p_ref.at[at], ext.at[at], in_sem.at[i])

    def landed(ref, sem):
        pltpu.make_async_copy(ref, ref, sem).wait()

    head = lax.select(ways[0] == 0, needs[0][0], needs[1][0])
    head_copy = take(pl.ds(head, 1), 0)
    head_copy.start()
    fetched[0].start()
    for flip in range(2):
        for way in range(2):

            @pl.when(ways[flip] == way)
            def _():
                for plane in needs[way][1 - flip :]:
                    take(pl.ds(plane, 1), 1 + flip).start()

    loads = []
    mid = nx - 11
    starts = (5, 5 + mid // 3, 5 + 2 * (mid // 3), nx - 6)
    for at, end in (*zip(starts[:-1], starts[1:], strict=True), (3, 4), (nx - 5, nx - 4)):
        loads.append(take(pl.ds(at, end - at), 3))
    for copy in loads:
        copy.start()
    for fetch in fetched[1:]:
        fetch.start()

    hops = doublings(n_row, n_col)

    def call(k):
        axis, far = hops[k]
        if axis:
            aim = ((row, away_c(far)), (row, away_c(-far)))
        else:
            aim = ((away_r(far), col), (away_r(-far), col))
        for to in aim:
            signal(hop_sem.at[k], *to)

    def relay(k):
        if k < len(hops):
            with jax.named_scope(f"r{k}"):
                pl.semaphore_wait(hop_sem.at[k], 2)
                if k + 1 < len(hops):
                    call(k + 1)

    def remote(i, j, src, dst, to):
        return pltpu.make_async_remote_copy(
            src_ref=src, dst_ref=dst, send_sem=h_send.at[i], recv_sem=h_recv.at[j],
            device_id=to, device_id_type=MESH,
        )

    def halo(piece, way):
        first, count = 0, 3
        if isinstance(piece, int) and piece in (0, 3):
            rows = pl.ds(TILE, ny - 2 * TILE)
            first, count = (1, 2) if piece else (0, 1)
            piece = 0
        else:
            rows = pl.ds(pl.multiple_of((piece - 1) * (ny - TILE), TILE), TILE)
        planes = lambda at: pl.ds(at + 3 * way + first, count)
        to = lax.rem(row + 1 + way * (n_row - 2), n_row)
        slot = piece if isinstance(piece, int) and piece == 0 else piece + way * (piece // 2)
        return remote(0, slot, yh.at[planes(0), rows], q.at[planes(nx), rows], (to, col))

    with jax.named_scope("wz"):
        alone = inner_twice(ny)
        fill_cyclic(wz_ref)
        sh[:, pl.ds(6, TILE - 6), :] = jnp.zeros((6, TILE - 6, nz), F32)
    def call_first():
        pl.semaphore_wait(barrier, 4)
        signal(last_sem, 0, col)

    with jax.named_scope("barl"):
        pl.when(at_last)(call_first)

    def prepare(way, flip):
        landed(ext.at[pl.ds(0, len(needs[way]) - 1 + flip)], in_sem.at[1 + flip])
        made = (partials_low, partials_high)[way]
        planes = made(lambda i: ext[i], *((nx,) if way == 0 else ()))
        for i, plane in enumerate(planes):
            hs[3 * way + i] = plane

    inside = ny - 2 * TILE
    inner_rows = pl.ds(TILE, inside)
    outer_rows = (pl.ds(0, TILE), pl.ds(ny - TILE, TILE))
    plane_rows = lambda way: hs[pl.ds(3 * way, 3)].reshape(3 * ny, nz)

    def lift_inner(way, data, first):
        count = 3 - first
        made = dot_pair(wx_ref[pl.ds(first * inside, count * inside)], data)
        yh[pl.ds(3 * way + first, count), inner_rows, :] = made.reshape(count, inside, nz)

    def lift_outer(way, data):
        made = dot_pair(wx_ref[pl.ds(3 * inside, 6 * TILE)], data).reshape(3, 2 * TILE, nz)
        for k, rows in enumerate(outer_rows):
            yh[pl.ds(3 * way, 3), rows, :] = made[:, k * TILE : (k + 1) * TILE, :]

    with jax.named_scope("hs0"):
        head_copy.wait()
    with jax.named_scope("lift0"):
        yh[3 * ways[0], inner_rows, :] = dot_pair(alone, ext[head])
    with jax.named_scope("bar"):
        pl.when(at_first)(lambda: pl.semaphore_wait(barrier, 3))
        pl.when(jnp.logical_not(at_first | at_last))(lambda: pl.semaphore_wait(barrier, 4))
    halo(0, ways[0]).start()
    with jax.named_scope("lift0b"):
        for way in range(2):
            pl.when(ways[0] == way)(lambda: prepare(way, 0))
        fetched[0].wait()
        lift_inner(ways[0], plane_rows(ways[0]), 1)
    halo(3, ways[0]).start()
    with jax.named_scope("hs1"):
        for way in range(2):
            pl.when(ways[1] == way)(lambda: prepare(way, 1))
        for i in range(6):
            line = lambda j: hs[i, pl.ds(j, 1), :]
            for k, one in enumerate(partials_low(line, ny) + partials_high(line)):
                sh[k, pl.ds(i, 1), :] = one
    lo, hi = pl.ds(0, 3), pl.ds(3, 3)
    for half_k, c in ((lo, up_c), (hi, dn_c)):
        remote(1, 4, sh.at[half_k], ch.at[half_k], (row, c)).start()
    if hops:
        call(0)
    with jax.named_scope("lift1"):
        lifted = dot2(plane_rows(ways[1]), wz_ref[...])
        lift_inner(ways[1], lifted, 0)

    def second():
        halo(0, ways[1]).start()
        halo(3, ways[1]).start()

    pl.when(jnp.logical_not(at_first))(second)

    far = lax.select(at_first, 1, lax.select(at_last, 0, odd_core))
    tail = (
        (1, far + odd_core - 2 * far * odd_core), (2 - odd_core, far),
        (1 + odd_core, odd_core * far + (1 - odd_core) * (1 - far)), (2, 1 - far),
    )
    groups = nx // grp

    def z_group(g):
        at = pl.ds(g * grp, grp)
        v = dot2(ext[at].reshape(grp * ny, nz), wz_ref[...])
        got = dot2(wy_ref[...], v)
        q[at] = got[: grp * ny].reshape(grp, ny, nz)
        su[:, at, :] = got[grp * ny :].reshape(6, grp, nz)
        for half_k, c in ((lo, up_c), (hi, dn_c)):
            remote(2, 5 + g, su.at[half_k, at], u.at[half_k, at], (row, c)).start()

    with jax.named_scope("ld2"):
        landed(ext.at[pl.ds(0, nx - len(sum(needs, ())))], in_sem.at[3])
        for fetch in fetched[1:]:
            fetch.wait()
    order = (0, groups - 1, *range(1, groups - 1))
    with jax.named_scope("z"):
        for g in order[: groups // 2]:
            z_group(g)
    with jax.named_scope("lift2"):
        lift_outer(ways[1], lifted)
        lift_outer(ways[0], dot2(plane_rows(ways[0]), wz_ref[...]))
    with jax.named_scope("last"):

        @pl.when(at_first)
        def _():
            pl.semaphore_wait(last_sem, 1)
            second()

    relay(0)
    with jax.named_scope("z2"):
        z_group(order[groups // 2])
    with jax.named_scope("wait_corner"):
        landed(ch, h_recv.at[4])
    with jax.named_scope("outer"):
        lifted = dot2(ch[...].reshape(6 * TILE, nz), wz_ref[...])
        more = dot_pair(wc_ref[...], lifted).reshape(6, 2 * TILE, nz)
        for k, rows in enumerate(outer_rows):
            yh[:, rows, :] += more[:, k * TILE : (k + 1) * TILE, :]
        for piece, way in tail:
            halo(piece, way).start()
    with jax.named_scope("z3"):
        for g in order[groups // 2 + 1 :]:
            z_group(g)
    relay(1)

    zb = cut_ref.shape[2]
    width = nz // zb
    n_lev = len(LEVELS)
    odd = lambda axis: lax.broadcasted_iota(jnp.int32, (TILE, LANES), axis) % 2
    mixed = (odd(0) + odd(1)) > 0

    def x_stage(totals, edges, first, last, sides=(1, 0)):
        totals = list(totals)
        for z in range(zb):
            cuts = jnp.full((TILE, LANES), -cut_ref[0, 0, z], jnp.int32)
            scale = jnp.exp2(cuts.astype(F32))
            limits = [level * scale for level in LEVELS]

            def tile(t, sums, z=z, limits=limits):
                rows = pl.ds(pl.multiple_of(t * TILE, TILE), TILE)
                sums = list(sums)
                for at in range(z * width, (z + 1) * width, LANES):
                    lanes = pl.ds(at, LANES)

                    def put(plane, value):
                        out_ref[plane, rows, lanes] = value
                        size = jnp.abs(value)
                        if plane % 2 == 0:
                            size = jnp.where(mixed, size, 0.0)
                        for n, limit in enumerate(limits):
                            sums[n] += jnp.maximum(size - limit, 0.0)

                    far = {-1: nx, half: nx + 3, half + 1: nx + 4}
                    e = lambda j: q[far.get(j, 2 * j), rows, lanes]

                    def detail(j):
                        if j == -1:
                            return q[nx + 1, rows, lanes] - 0.5625 * e(0) + 0.0625 * e(1)
                        if j == -2:
                            return q[nx + 2, rows, lanes] + 0.0625 * e(0)
                        if j == half:
                            return q[nx + 5, rows, lanes] + 0.0625 * e(half - 1)
                        return q[2 * j + 1, rows, lanes] - 0.5625 * (e(j) + e(j + 1)) + 0.0625 * (e(j - 1) + e(j + 2))

                    def smooth(d, j):
                        put(2 * j, e(j) + 0.28125 * (d[j - 1] + d[j]) - 0.03125 * (d[j - 2] + d[j + 1]))

                    if not edges:
                        d = {}
                        for j in range(1, half - 2):
                            d[j] = detail(j)
                            put(2 * j + 1, d[j])
                            if j >= 4:
                                smooth(d, j - 1)
                    if edges and 0 in sides:
                        d = {j: out_ref[2 * j + 1, rows, lanes] for j in (1, 2, 3)}
                        d |= {j: detail(j) for j in (-2, -1, 0)}
                        put(1, d[0])
                        for j in (0, 1, 2):
                            smooth(d, j)
                    if edges and 1 in sides:
                        d = {j: out_ref[2 * j + 1, rows, lanes] for j in range(half - 5, half - 2)}
                        d |= {j: detail(j) for j in range(half - 2, half + 1)}
                        for j in (half - 2, half - 1):
                            put(2 * j + 1, d[j])
                        for j in range(half - 3, half):
                            smooth(d, j)
                return tuple(sums)

            mine = slice(z * n_lev, (z + 1) * n_lev)
            totals[mine] = lax.fori_loop(first, last, tile, tuple(totals[mine]))
        return totals

    tiles = ny // TILE
    totals = [jnp.zeros((TILE, LANES), F32) for _ in range(zb * n_lev)]
    with jax.named_scope("xin"):
        totals = x_stage(totals, False, 1, tiles - 1)
    relay(2)
    with jax.named_scope("wait_inner"):
        landed(q.at[pl.ds(nx, 6), inner_rows], h_recv.at[0])

        def make_up(way):
            at = pl.ds(nx + 3 * way, 3)
            raw = q[at, inner_rows, :].reshape(3 * inside, nz)
            q[at, inner_rows, :] = dot2(raw, wz_ref[...]).reshape(3, inside, nz)

        pl.when(first_way(dn_r) == 0)(lambda: make_up(0))
        pl.when(first_way(up_r) == 1)(lambda: make_up(1))
    with jax.named_scope("xinner"):
        totals = x_stage(totals, True, 1, tiles - 1)
    for g in order:
        with jax.named_scope("wait_u"):
            landed(u.at[:, pl.ds(g * grp, grp)], h_recv.at[5 + g])
        with jax.named_scope("u"):
            at = pl.ds(g * grp, grp)
            more = dot_pair(wu_ref[...], u[:, at, :].reshape(6 * grp, nz))
            more = more.reshape(grp, 2 * TILE, nz)
            for k, rows in enumerate(outer_rows):
                q[at, rows, :] += more[:, k * TILE : (k + 1) * TILE, :]
    for k in range(3, len(hops)):
        relay(k)
    with jax.named_scope("xin2"):
        for t in (0, tiles - 1):
            totals = x_stage(totals, False, t, t + 1)
    with jax.named_scope("wait_outer"):
        landed(q.at[pl.ds(nx, 6), outer_rows[0]], h_recv.at[1])
    with jax.named_scope("xouter"):
        totals = x_stage(totals, True, 0, 1)
    for way in (1, 0):
        with jax.named_scope("wait_outer"):
            landed(q.at[pl.ds(nx + 3 * way, 3), outer_rows[1]], h_recv.at[2 + way])
        with jax.named_scope("xouter"):
            totals = x_stage(totals, True, tiles - 1, tiles, (way,))
    with jax.named_scope("line"):
        rows = zb * n_lev
        lane, at = (lax.broadcasted_iota(jnp.int32, (rows, LANES), axis) for axis in (1, 0))
        group = jnp.full((rows, LANES), map_ref[0, 0, 0], jnp.int32)
        for z in range(1, zb):
            group = jnp.where(at >= z * n_lev, map_ref[0, 0, z], group)
        sums = jnp.concatenate([jnp.sum(total, axis=0, keepdims=True) for total in totals], 0)
        mass = jnp.sum(sums, axis=1, keepdims=True) / (nx * ny * width)
        line = jnp.where(lane == at % n_lev * GROUPS + group, mass, 0.0)
        line = jnp.sum(line, axis=0, keepdims=True)
        part[...] = line
        slots[me] = line

    def spread(r, c):
        pltpu.make_async_remote_copy(
            src_ref=part, dst_ref=slots.at[me], send_sem=g_sem.at[0],
            recv_sem=g_sem.at[1], device_id=(r, c), device_id_type=MESH,
        ).start()

    def peers(visit):
        if devices <= UNROLL:
            for j in (*range(1, n_row), 0):
                for k in range(n_col):
                    if j or k:
                        visit(away_r(j), away_c(k))
            return

        @pl.loop(1, n_row)
        def _(j):
            @pl.loop(0, n_col)
            def _(k):
                visit(lax.rem(row + j, n_row), lax.rem(col + k, n_col))

        @pl.loop(1, n_col)
        def _(k):
            visit(row, lax.rem(col + k, n_col))

    with jax.named_scope("spread"):
        peers(spread)
    with jax.named_scope("wsend"):
        for i, sent in enumerate((yh, sh, su)):
            landed(sent, h_send.at[i])
    with jax.named_scope("gather"):
        for i in range(2):
            landed(slots.at[pl.ds(0, devices - 1)], g_sem.at[i])
    mass_ref[...] = slots[...]


def deliver(c_ref, m_ref, out_hbm, mass_hbm, mass, sems, m_sem):
    count = sems.shape[0]
    size = c_ref.shape[0] // count
    copies = []
    for i in range(count):
        at = pl.ds(i * size, size)
        copies.append(pltpu.make_async_copy(c_ref.at[at], out_hbm.at[at], sems.at[i]))
        copies[i].start()
    total = jnp.sum(m_ref[...], axis=0)
    mass[...] = jnp.concatenate(
        [total[:, n * GROUPS : (n + 1) * GROUPS] for n in range(len(LEVELS))], 0
    )
    copies.append(pltpu.make_async_copy(mass, mass_hbm, m_sem))
    copies[-1].start()
    for copy in copies:
        copy.wait()


def solution(mesh):
    n_row, n_col = mesh.shape["row"], mesh.shape["col"]

    def shards(pressure, cut_exponent, group_map):
        nx, ny, nz = pressure.shape
        grp = 8
        devices = n_row * n_col
        local = local_matrix(ny)
        own, beyond = local[:, :ny], local[:, ny:]
        eye = np.eye(ny)
        take = lambda i: eye[i]
        near = np.stack(partials_low(take, ny) + partials_high(take))
        ws = np.einsum("ky,xw->kxwy", near, np.eye(grp)).reshape(6 * grp, grp * ny)
        wy = np.concatenate([np.kron(np.eye(grp), own), ws])
        rim = np.r_[0:TILE, ny - TILE : ny]
        spread = lambda planes: np.einsum("wp,yk->pykw", planes, beyond[rim]).reshape(
            planes.shape[1] * 2 * TILE, -1
        )
        core = np.r_[TILE : ny - TILE]
        twice = lambda w: np.tile(w, 2)
        wx = np.concatenate([twice(np.kron(np.eye(3), own[rows])) for rows in (core, rim)])
        wc, wu = spread(np.eye(TILE, 6)), spread(np.eye(grp))
        wide = lambda w: np.pad(w, ((0, 0), (0, wy.shape[1] - w.shape[1])))
        wall = np.concatenate([wy, wide(twice(wc)), wide(twice(wu))])
        weights = [jnp.asarray(w, BF16) for w in (wx, wall)]
        vmem = pl.BlockSpec(memory_space=pltpu.VMEM)
        hbm = pl.BlockSpec(memory_space=pltpu.HBM)
        hops = len(doublings(n_row, n_col))
        found = pl.pallas_call(
            functools.partial(kernel, n_row, n_col, grp),
            out_shape=(
                pltpu.VMEM((nx, ny, nz), F32),
                pltpu.VMEM((devices, 1, LANES), F32),
            ),
            in_specs=[hbm] * (3 + len(weights)),
            out_specs=(vmem, vmem),
            scratch_shapes=[
                pltpu.VMEM((nx, ny, nz), F32),
                pltpu.VMEM((nx + 6, ny, nz), F32),
                pltpu.VMEM((6, ny, nz), F32),
                pltpu.VMEM((6, ny, nz), F32),
                pltpu.VMEM((6, TILE, nz), F32),
                pltpu.VMEM((6, TILE, nz), F32),
                pltpu.VMEM((6, nx, nz), F32),
                pltpu.VMEM((6, nx, nz), F32),
                pltpu.VMEM((1, LANES), F32),
                pltpu.VMEM((devices, 1, LANES), F32),
                pltpu.SMEM(cut_exponent.shape, jnp.int32),
                pltpu.SMEM(group_map.shape, jnp.int32),
                pltpu.VMEM((nz, nz), BF16),
                *(pltpu.VMEM(w.shape, BF16) for w in weights),
                pltpu.SemaphoreType.DMA((4,)),
                pltpu.SemaphoreType.DMA((len(weights) + 2,)),
                pltpu.SemaphoreType.DMA((3,)),
                pltpu.SemaphoreType.DMA((5 + nx // grp,)),
                pltpu.SemaphoreType.DMA((2,)),
                pltpu.SemaphoreType.REGULAR((max(hops, 1),)),
                pltpu.SemaphoreType.REGULAR,
            ],
            compiler_params=pltpu.CompilerParams(
                collective_id=0, has_side_effects=True, vmem_limit_bytes=24 * 2**20
            ),
        )(*(pltpu.with_memory_space_constraint(x, pltpu.HBM) for x in (cut_exponent, group_map, pressure, *weights)))
        coeffs, mass = pl.pallas_call(
            deliver,
            out_shape=(
                pltpu.HBM((nx, ny, nz), F32), pltpu.HBM((len(LEVELS), GROUPS), F32),
            ),
            in_specs=[vmem] * 2,
            out_specs=(hbm, hbm),
            scratch_shapes=[
                pltpu.VMEM((len(LEVELS), GROUPS), F32),
                pltpu.SemaphoreType.DMA((1,)),
                pltpu.SemaphoreType.DMA,
            ],
            compiler_params=pltpu.CompilerParams(vmem_limit_bytes=2**20),
        )(*(pltpu.with_memory_space_constraint(x, pltpu.VMEM) for x in found))
        return coeffs, mass.T

    specs = P("row", "col", None)
    return jax.shard_map(
        shards, mesh=mesh, in_specs=(specs,) * 3, out_specs=(specs, P()), check_vma=False
    )
```

```python
import functools

import jax
import jax.numpy as jnp
import numpy as np
from jax import lax
from jax.experimental import pallas as pl
from jax.experimental.pallas import tpu as pltpu
from jax.sharding import PartitionSpec as P

GROUPS = 16
LEVELS = (0.25, 0.5, 1.0, 2.0)
MESH = pl.DeviceIdType.MESH
F32, BF16 = jnp.float32, jnp.bfloat16
TILE, LANES = 8, 128
UNROLL = 64


def cyclic_matrix(n):
    ev, od = np.eye(n)[0::2], np.eye(n)[1::2]
    r = lambda a, k: np.roll(a, k, 0)
    d = od - (0.5625 * (ev + r(ev, -1)) - 0.0625 * (r(ev, 1) + r(ev, -2)))
    s = ev + (0.28125 * (r(d, 1) + d) - 0.03125 * (r(d, 2) + r(d, -1)))
    return np.stack([s, d], 1).reshape(n, n)


def local_matrix(n):
    half = n // 2
    t = np.eye(n + 6)
    v, (a, b, c, f0, f1, g) = t[:n], t[n:]
    e = {j: v[2 * j] for j in range(half)}
    o = {j: v[2 * j + 1] for j in range(half)}
    e[-1], e[half], e[half + 1] = a, f0, f1
    d = {
        j: o[j] - 0.5625 * (e[j] + e[j + 1]) + 0.0625 * (e[j - 1] + e[j + 2])
        for j in range(half)
    }
    d[-1] = b - 0.5625 * e[0] + 0.0625 * e[1]
    d[-2] = c + 0.0625 * e[0]
    d[half] = g + 0.0625 * e[half - 1]
    out = np.zeros((n, n + 6))
    for j in range(half):
        out[2 * j] = e[j] + 0.28125 * (d[j - 1] + d[j]) - 0.03125 * (d[j - 2] + d[j + 1])
        out[2 * j + 1] = d[j]
    return out


def partials_low(row, n):
    a = row(n - 2)
    b = row(n - 1) - 0.5625 * a + 0.0625 * row(n - 4)
    c = row(n - 3) - 0.5625 * (row(n - 4) + a) + 0.0625 * row(n - 6)
    return a, b, c


def partials_high(row):
    f0, f1 = row(0), row(2)
    return f0, f1, row(1) - 0.5625 * (f0 + f1) + 0.0625 * row(4)


def split(value):
    hi = value.astype(BF16)
    return hi, (value - hi.astype(F32)).astype(BF16)


def dot2(left, right):
    dot = functools.partial(jnp.dot, preferred_element_type=F32)
    if left.dtype == BF16:
        hi, lo = split(right)
        return dot(left, hi) + dot(left, lo)
    hi, lo = split(left)
    return dot(hi, right) + dot(lo, right)


def dot_pair(left, right):
    return jnp.dot(left, jnp.concatenate(split(right), 0), preferred_element_type=F32)


def doublings(n_row, n_col):
    hops, known = [], 1
    while known < n_col // 2:
        hops.append((1, known))
        known *= 2
    known = 0
    while known < n_row // 2:
        hops.append((0, max(known, 1)))
        known += max(known, 1)
    return hops


def band(first_row, coefs):
    shape = (2 * TILE, LANES)
    lane = lax.broadcasted_iota(jnp.int32, shape, 1)
    far = jnp.abs(lane - lax.broadcasted_iota(jnp.int32, shape, 0) + first_row)
    value = jnp.zeros(shape, F32)
    for k, (even, odd) in enumerate(coefs):
        if even or odd:
            value = jnp.where(far == k, jnp.where(lane % 2 == 1, odd, even), value)
    return value.astype(BF16)


def inner_twice(n):
    shape = (n - 2 * TILE, 2 * n)
    row, cell = (lax.broadcasted_iota(jnp.int32, shape, axis) for axis in (0, 1))
    far = jnp.abs(cell % n - row - TILE)
    value = jnp.zeros(shape, F32)
    for k, (even, odd) in enumerate(coefficients(n)):
        value = jnp.where(far == k, jnp.where(row % 2 == 1, odd, even), value)
    return value.astype(BF16)


def coefficients(n):
    full = cyclic_matrix(n)
    return [(float(full[0, k]), float(full[1, 1 + k])) for k in range(7)]


def fill_cyclic(ref):
    n = ref.shape[0]
    coefs = coefficients(n)
    reach = len(coefs)
    made = {}
    for r in range(0, n, 2 * TILE):
        for c in range(0, n, LANES):
            off = (c - r + n // 2) % n - n // 2
            near = off - 2 * TILE < reach and off + LANES > -reach
            key = off if near else None
            if key not in made:
                made[key] = band(off, coefs) if near else jnp.zeros((2 * TILE, LANES), BF16)
            ref[pl.ds(r, 2 * TILE), pl.ds(c, LANES)] = made[key]


def kernel(n_row, n_col, grp, cut_hbm, map_hbm, p_ref, *refs):
    weights, refs = refs[:2], refs[2:]
    out_ref, mass_ref = refs[:2]
    ext, q, hs, yh, ch, su, u, part, slots, block_ref, wz_ref = refs[2:13]
    held = refs[13:15]
    wx_ref, wall_ref = held
    in_sem, w_sem, h_send, h_recv, g_sem, hop_sem, last_sem = refs[15:]
    nx, ny, nz = p_ref.shape
    half = nx // 2
    tall = grp * ny + 6 * grp
    wy_ref = wall_ref.at[pl.ds(0, tall)]
    wc_ref = wall_ref.at[pl.ds(tall, 12 * TILE), pl.ds(0, 12 * TILE)]
    wu_ref = wall_ref.at[pl.ds(tall + 12 * TILE, 2 * TILE * grp), pl.ds(0, 12 * grp)]
    devices = n_row * n_col
    row, col = lax.axis_index("row"), lax.axis_index("col")
    me = row * n_col + col
    away_r = lambda k: lax.rem(row + (k + n_row), n_row)
    away_c = lambda k: lax.rem(col + (k + n_col), n_col)
    up_r, dn_r, up_c, dn_c = away_r(1), away_r(-1), away_c(1), away_c(-1)

    barrier = pltpu.get_barrier_semaphore()
    top = n_row - 1
    at_first, at_last = row == 0, row == top

    def signal(sem, r, c):
        pl.semaphore_signal(sem, inc=1, device_id=(r, c), device_id_type=MESH)

    for r, c in ((dn_r, col), (row, up_c), (row, dn_c)):
        signal(barrier, r, c)
    pl.when(jnp.logical_not(at_last))(lambda: signal(barrier, row + 1, col))

    fetched = [
        pltpu.make_async_copy(src, dst, w_sem.at[i])
        for i, (src, dst) in enumerate(zip(weights, held, strict=True))
    ]
    odd_core = lax.rem(col, 2)

    def first_way(r):
        return lax.select(r == 0, 0, odd_core)

    ways = (first_way(row), 1 - first_way(row))
    needs = ((nx - 2, nx - 1, nx - 4, nx - 3, nx - 6), (0, 2, 1, 4))

    def take(at, i):
        return pltpu.make_async_copy(p_ref.at[at], ext.at[at], in_sem.at[i])

    def landed(ref, sem):
        pltpu.make_async_copy(ref, ref, sem).wait()

    head = lax.select(ways[0] == 0, needs[0][0], needs[1][0])
    head_copy = take(pl.ds(head, 1), 0)
    head_copy.start()
    fetched[0].start()
    for flip in range(2):
        for way in range(2):

            @pl.when(ways[flip] == way)
            def _():
                for plane in needs[way][1 - flip :]:
                    take(pl.ds(plane, 1), 1 + flip).start()

    loads = []
    mid = nx - 11
    starts = (5, 5 + mid // 3, 5 + 2 * (mid // 3), nx - 6)
    for at, end in (*zip(starts[:-1], starts[1:], strict=True), (3, 4), (nx - 5, nx - 4)):
        loads.append(take(pl.ds(at, end - at), 3))
    for copy in loads:
        copy.start()
    for fetch in fetched[1:]:
        fetch.start()
    for src, i in ((cut_hbm, 0), (map_hbm, 1)):
        pltpu.make_async_copy(src, block_ref.at[pl.ds(i, 1)], w_sem.at[2]).start()

    hops = doublings(n_row, n_col)

    def call(k):
        axis, far = hops[k]
        if axis:
            aim = ((row, away_c(far)), (row, away_c(-far)))
        else:
            aim = ((away_r(far), col), (away_r(-far), col))
        for to in aim:
            signal(hop_sem.at[k], *to)

    def relay(k):
        if k < len(hops):
            with jax.named_scope(f"r{k}"):
                pl.semaphore_wait(hop_sem.at[k], 2)
                if k + 1 < len(hops):
                    call(k + 1)

    def remote(i, j, src, dst, to):
        return pltpu.make_async_remote_copy(
            src_ref=src, dst_ref=dst, send_sem=h_send.at[i], recv_sem=h_recv.at[j],
            device_id=to, device_id_type=MESH,
        )

    def halo(piece, way):
        first, count = 0, 3
        if isinstance(piece, int) and piece in (0, 3):
            rows = pl.ds(TILE, ny - 2 * TILE)
            first, count = (1, 2) if piece else (0, 1)
            piece = 0
        else:
            rows = pl.ds(pl.multiple_of((piece - 1) * (ny - TILE), TILE), TILE)
        planes = lambda at: pl.ds(at + 3 * way + first, count)
        to = lax.rem(row + 1 + way * (n_row - 2), n_row)
        slot = piece if isinstance(piece, int) and piece == 0 else piece + way * (piece // 2)
        return remote(0, slot, yh.at[planes(0), rows], q.at[planes(nx), rows], (to, col))

    with jax.named_scope("wz"):
        alone = inner_twice(ny)
        fill_cyclic(wz_ref)
        su[:, pl.ds(nx + 6, TILE - 6), :] = jnp.zeros((6, TILE - 6, nz), F32)
    def call_first():
        pl.semaphore_wait(barrier, 4)
        signal(last_sem, 0, col)

    with jax.named_scope("barl"):
        pl.when(at_last)(call_first)

    def prepare(way, flip):
        landed(ext.at[pl.ds(0, len(needs[way]) - 1 + flip)], in_sem.at[1 + flip])
        made = (partials_low, partials_high)[way]
        planes = made(lambda i: ext[i], *((nx,) if way == 0 else ()))
        for i, plane in enumerate(planes):
            hs[3 * way + i] = plane

    inside = ny - 2 * TILE
    inner_rows = pl.ds(TILE, inside)
    outer_rows = (pl.ds(0, TILE), pl.ds(ny - TILE, TILE))
    plane_rows = lambda way: hs[pl.ds(3 * way, 3)].reshape(3 * ny, nz)

    def lift_inner(way, data, first):
        count = 3 - first
        made = dot_pair(wx_ref[pl.ds(first * inside, count * inside)], data)
        yh[pl.ds(3 * way + first, count), inner_rows, :] = made.reshape(count, inside, nz)

    def lift_outer(way, data):
        made = dot_pair(wx_ref[pl.ds(3 * inside, 6 * TILE)], data).reshape(3, 2 * TILE, nz)
        for k, rows in enumerate(outer_rows):
            yh[pl.ds(3 * way, 3), rows, :] = made[:, k * TILE : (k + 1) * TILE, :]

    with jax.named_scope("hs0"):
        head_copy.wait()
    with jax.named_scope("lift0"):
        yh[3 * ways[0], inner_rows, :] = dot_pair(alone, ext[head])
    with jax.named_scope("bar"):
        pl.when(at_first)(lambda: pl.semaphore_wait(barrier, 3))
        pl.when(jnp.logical_not(at_first | at_last))(lambda: pl.semaphore_wait(barrier, 4))
    halo(0, ways[0]).start()
    with jax.named_scope("lift0b"):
        for way in range(2):
            pl.when(ways[0] == way)(lambda: prepare(way, 0))
        fetched[0].wait()
        lift_inner(ways[0], plane_rows(ways[0]), 1)
    halo(3, ways[0]).start()
    with jax.named_scope("hs1"):
        for way in range(2):
            pl.when(ways[1] == way)(lambda: prepare(way, 1))
        for i in range(6):
            line = lambda j: hs[i, pl.ds(j, 1), :]
            for k, one in enumerate(partials_low(line, ny) + partials_high(line)):
                su[k, pl.ds(nx + i, 1), :] = one
    lo, hi = pl.ds(0, 3), pl.ds(3, 3)
    for half_k, c in ((lo, up_c), (hi, dn_c)):
        remote(1, 4, su.at[half_k, pl.ds(nx, TILE)], ch.at[half_k], (row, c)).start()
    if hops:
        call(0)
    with jax.named_scope("lift1"):
        lifted = dot2(plane_rows(ways[1]), wz_ref[...])
        lift_inner(ways[1], lifted, 0)

    def second():
        halo(0, ways[1]).start()
        halo(3, ways[1]).start()

    pl.when(jnp.logical_not(at_first))(second)

    far = lax.select(at_first, 1, lax.select(at_last, 0, odd_core))
    tail = (
        (1, far + odd_core - 2 * far * odd_core), (2 - odd_core, far),
        (1 + odd_core, odd_core * far + (1 - odd_core) * (1 - far)), (2, 1 - far),
    )
    groups = nx // grp
    order = (0, groups - 1, *range(1, groups - 1))

    def z_group(g):
        at = pl.ds(g * grp, grp)
        v = dot2(ext[at].reshape(grp * ny, nz), wz_ref[...])
        got = dot2(wy_ref[...], v)
        q[at] = got[: grp * ny].reshape(grp, ny, nz)
        su[:, at, :] = got[grp * ny :].reshape(6, grp, nz)
        for half_k, c in ((lo, up_c), (hi, dn_c)):
            remote(1, 5 + (g == order[-1]), su.at[half_k, at], u.at[half_k, at], (row, c)).start()

    with jax.named_scope("ld2"):
        landed(ext.at[pl.ds(0, nx - len(sum(needs, ())))], in_sem.at[3])
        for fetch in fetched[1:]:
            fetch.wait()
        landed(block_ref, w_sem.at[2])
    with jax.named_scope("z"):
        for g in order[: groups // 2]:
            z_group(g)
    with jax.named_scope("last"):

        @pl.when(at_first)
        def _():
            pl.semaphore_wait(last_sem, 1)
            second()

    with jax.named_scope("lift2"):
        lift_outer(ways[1], lifted)
        lift_outer(ways[0], dot2(plane_rows(ways[0]), wz_ref[...]))
    relay(0)
    with jax.named_scope("z2"):
        z_group(order[groups // 2])
    with jax.named_scope("wait_corner"):
        landed(ch, h_recv.at[4])
    with jax.named_scope("outer"):
        lifted = dot2(ch[...].reshape(6 * TILE, nz), wz_ref[...])
        more = dot_pair(wc_ref[...], lifted).reshape(6, 2 * TILE, nz)
        for k, rows in enumerate(outer_rows):
            yh[:, rows, :] += more[:, k * TILE : (k + 1) * TILE, :]
        for piece, way in tail:
            halo(piece, way).start()
    with jax.named_scope("z3"):
        for g in order[groups // 2 + 1 :]:
            z_group(g)
    relay(1)

    zb = block_ref.shape[2]
    width = nz // zb
    n_lev = len(LEVELS)
    odd = lambda axis: lax.broadcasted_iota(jnp.int32, (TILE, LANES), axis) % 2
    mixed = (odd(0) + odd(1)) > 0

    def x_stage(totals, edges, first, last, sides=(1, 0)):
        totals = list(totals)
        for z in range(zb):
            cuts = jnp.full((TILE, LANES), -block_ref[0, 0, z], jnp.int32)
            scale = jnp.exp2(cuts.astype(F32))
            limits = [level * scale for level in LEVELS]

            def tile(t, sums, z=z, limits=limits):
                rows = pl.ds(pl.multiple_of(t * TILE, TILE), TILE)
                sums = list(sums)
                for at in range(z * width, (z + 1) * width, LANES):
                    lanes = pl.ds(at, LANES)

                    def put(plane, value):
                        out_ref[plane, rows, lanes] = value
                        size = jnp.abs(value)
                        if plane % 2 == 0:
                            size = jnp.where(mixed, size, 0.0)
                        for n, limit in enumerate(limits):
                            sums[n] += jnp.maximum(size - limit, 0.0)

                    far = {-1: nx, half: nx + 3, half + 1: nx + 4}
                    e = lambda j: q[far.get(j, 2 * j), rows, lanes]

                    def detail(j):
                        if j == -1:
                            return q[nx + 1, rows, lanes] - 0.5625 * e(0) + 0.0625 * e(1)
                        if j == -2:
                            return q[nx + 2, rows, lanes] + 0.0625 * e(0)
                        if j == half:
                            return q[nx + 5, rows, lanes] + 0.0625 * e(half - 1)
                        return q[2 * j + 1, rows, lanes] - 0.5625 * (e(j) + e(j + 1)) + 0.0625 * (e(j - 1) + e(j + 2))

                    def smooth(d, j):
                        put(2 * j, e(j) + 0.28125 * (d[j - 1] + d[j]) - 0.03125 * (d[j - 2] + d[j + 1]))

                    if not edges:
                        d = {}
                        for j in range(1, half - 2):
                            d[j] = detail(j)
                            put(2 * j + 1, d[j])
                            if j >= 4:
                                smooth(d, j - 1)
                    if edges and 0 in sides:
                        d = {j: out_ref[2 * j + 1, rows, lanes] for j in (1, 2, 3)}
                        d |= {j: detail(j) for j in (-2, -1, 0)}
                        put(1, d[0])
                        for j in (0, 1, 2):
                            smooth(d, j)
                    if edges and 1 in sides:
                        d = {j: out_ref[2 * j + 1, rows, lanes] for j in range(half - 5, half - 2)}
                        d |= {j: detail(j) for j in range(half - 2, half + 1)}
                        for j in (half - 2, half - 1):
                            put(2 * j + 1, d[j])
                        for j in range(half - 3, half):
                            smooth(d, j)
                return tuple(sums)

            mine = slice(z * n_lev, (z + 1) * n_lev)
            totals[mine] = lax.fori_loop(first, last, tile, tuple(totals[mine]))
        return totals

    tiles = ny // TILE
    totals = [jnp.zeros((TILE, LANES), F32) for _ in range(zb * n_lev)]
    with jax.named_scope("xin"):
        totals = x_stage(totals, False, 1, tiles - 1)
    relay(2)
    with jax.named_scope("wait_inner"):
        landed(q.at[pl.ds(nx, 6), inner_rows], h_recv.at[0])

        def make_up(way):
            at = pl.ds(nx + 3 * way, 3)
            raw = q[at, inner_rows, :].reshape(3 * inside, nz)
            q[at, inner_rows, :] = dot2(raw, wz_ref[...]).reshape(3, inside, nz)

        pl.when(first_way(dn_r) == 0)(lambda: make_up(0))
        pl.when(first_way(up_r) == 1)(lambda: make_up(1))
    with jax.named_scope("xinner"):
        totals = x_stage(totals, True, 1, tiles - 1)
    for g in order:
        with jax.named_scope("wait_u"):
            if g in (order[0], order[-1]):
                count = 1 if g == order[-1] else groups - 1
                landed(u.at[:, pl.ds(0, count * grp)], h_recv.at[6 - (count > 1)])
        with jax.named_scope("u"):
            at = pl.ds(g * grp, grp)
            more = dot_pair(wu_ref[...], u[:, at, :].reshape(6 * grp, nz))
            more = more.reshape(grp, 2 * TILE, nz)
            for k, rows in enumerate(outer_rows):
                q[at, rows, :] += more[:, k * TILE : (k + 1) * TILE, :]
    for k in range(3, len(hops)):
        relay(k)
    with jax.named_scope("xin2"):
        for t in (0, tiles - 1):
            totals = x_stage(totals, False, t, t + 1)
    with jax.named_scope("wait_outer"):
        landed(q.at[pl.ds(nx, 6), outer_rows[0]], h_recv.at[1])
    with jax.named_scope("xouter"):
        totals = x_stage(totals, True, 0, 1)
    for way in (1, 0):
        with jax.named_scope("wait_outer"):
            landed(q.at[pl.ds(nx + 3 * way, 3), outer_rows[1]], h_recv.at[2 + way])
        with jax.named_scope("xouter"):
            totals = x_stage(totals, True, tiles - 1, tiles, (way,))
    with jax.named_scope("line"):
        rows = zb * n_lev
        lane, at = (lax.broadcasted_iota(jnp.int32, (rows, LANES), axis) for axis in (1, 0))
        group = jnp.full((rows, LANES), block_ref[1, 0, 0], jnp.int32)
        for z in range(1, zb):
            group = jnp.where(at >= z * n_lev, block_ref[1, 0, z], group)
        sums = jnp.concatenate([jnp.sum(total, axis=0, keepdims=True) for total in totals], 0)
        mass = jnp.sum(sums, axis=1, keepdims=True) / (nx * ny * width)
        line = jnp.where(lane == at % n_lev * GROUPS + group, mass, 0.0)
        line = jnp.sum(line, axis=0, keepdims=True)
        part[...] = line
        slots[me] = line

    def spread(r, c):
        pltpu.make_async_remote_copy(
            src_ref=part, dst_ref=slots.at[me], send_sem=g_sem.at[0],
            recv_sem=g_sem.at[1], device_id=(r, c), device_id_type=MESH,
        ).start()

    def peers(visit):
        if devices <= UNROLL:
            for j in (*range(1, n_row), 0):
                for k in range(n_col):
                    if j or k:
                        visit(away_r(j), away_c(k))
            return

        @pl.loop(1, n_row)
        def _(j):
            @pl.loop(0, n_col)
            def _(k):
                visit(lax.rem(row + j, n_row), lax.rem(col + k, n_col))

        @pl.loop(1, n_col)
        def _(k):
            visit(row, lax.rem(col + k, n_col))

    with jax.named_scope("spread"):
        peers(spread)
    with jax.named_scope("wsend"):
        for i, sent in enumerate((yh, su)):
            landed(sent, h_send.at[i])
    with jax.named_scope("gather"):
        for i in range(2):
            landed(slots.at[pl.ds(0, devices - 1)], g_sem.at[i])
    mass_ref[...] = slots[...]


def deliver(c_ref, m_ref, out_hbm, mass_hbm, mass, sems, m_sem):
    count = sems.shape[0]
    size = c_ref.shape[0] // count
    copies = []
    for i in range(count):
        at = pl.ds(i * size, size)
        copies.append(pltpu.make_async_copy(c_ref.at[at], out_hbm.at[at], sems.at[i]))
        copies[i].start()
    total = jnp.sum(m_ref[...], axis=0)
    mass[...] = jnp.concatenate(
        [total[:, n * GROUPS : (n + 1) * GROUPS] for n in range(len(LEVELS))], 0
    )
    copies.append(pltpu.make_async_copy(mass, mass_hbm, m_sem))
    copies[-1].start()
    for copy in copies:
        copy.wait()


def solution(mesh):
    n_row, n_col = mesh.shape["row"], mesh.shape["col"]

    def shards(pressure, cut_exponent, group_map):
        nx, ny, nz = pressure.shape
        grp = 8
        devices = n_row * n_col
        local = local_matrix(ny)
        own, beyond = local[:, :ny], local[:, ny:]
        eye = np.eye(ny)
        take = lambda i: eye[i]
        near = np.stack(partials_low(take, ny) + partials_high(take))
        ws = np.einsum("ky,xw->kxwy", near, np.eye(grp)).reshape(6 * grp, grp * ny)
        wy = np.concatenate([np.kron(np.eye(grp), own), ws])
        rim = np.r_[0:TILE, ny - TILE : ny]
        spread = lambda planes: np.einsum("wp,yk->pykw", planes, beyond[rim]).reshape(
            planes.shape[1] * 2 * TILE, -1
        )
        core = np.r_[TILE : ny - TILE]
        twice = lambda w: np.tile(w, 2)
        wx = np.concatenate([twice(np.kron(np.eye(3), own[rows])) for rows in (core, rim)])
        wc, wu = spread(np.eye(TILE, 6)), spread(np.eye(grp))
        wide = lambda w: np.pad(w, ((0, 0), (0, wy.shape[1] - w.shape[1])))
        wall = np.concatenate([wy, wide(twice(wc)), wide(twice(wu))])
        weights = [jnp.asarray(w, BF16) for w in (wx, wall)]
        vmem = pl.BlockSpec(memory_space=pltpu.VMEM)
        hbm = pl.BlockSpec(memory_space=pltpu.HBM)
        hops = len(doublings(n_row, n_col))
        found = pl.pallas_call(
            functools.partial(kernel, n_row, n_col, grp),
            out_shape=(
                pltpu.VMEM((nx, ny, nz), F32),
                pltpu.VMEM((devices, 1, LANES), F32),
            ),
            in_specs=[hbm] * (3 + len(weights)),
            out_specs=(vmem, vmem),
            scratch_shapes=[
                pltpu.VMEM((nx, ny, nz), F32),
                pltpu.VMEM((nx + 6, ny, nz), F32),
                pltpu.VMEM((6, ny, nz), F32),
                pltpu.VMEM((6, ny, nz), F32),
                pltpu.VMEM((6, TILE, nz), F32),
                pltpu.VMEM((6, nx + TILE, nz), F32),
                pltpu.VMEM((6, nx, nz), F32),
                pltpu.VMEM((1, LANES), F32),
                pltpu.VMEM((devices, 1, LANES), F32),
                pltpu.SMEM((2, *cut_exponent.shape[1:]), jnp.int32),
                pltpu.VMEM((nz, nz), BF16),
                *(pltpu.VMEM(w.shape, BF16) for w in weights),
                pltpu.SemaphoreType.DMA((4,)),
                pltpu.SemaphoreType.DMA((len(weights) + 1,)),
                pltpu.SemaphoreType.DMA((2,)),
                pltpu.SemaphoreType.DMA((7,)),
                pltpu.SemaphoreType.DMA((2,)),
                pltpu.SemaphoreType.REGULAR((max(hops, 1),)),
                pltpu.SemaphoreType.REGULAR,
            ],
            compiler_params=pltpu.CompilerParams(
                collective_id=0, has_side_effects=True, vmem_limit_bytes=24 * 2**20
            ),
        )(*(pltpu.with_memory_space_constraint(x, pltpu.HBM) for x in (cut_exponent, group_map, pressure, *weights)))
        coeffs, mass = pl.pallas_call(
            deliver,
            out_shape=(
                pltpu.HBM((nx, ny, nz), F32), pltpu.HBM((len(LEVELS), GROUPS), F32),
            ),
            in_specs=[vmem] * 2,
            out_specs=(hbm, hbm),
            scratch_shapes=[
                pltpu.VMEM((len(LEVELS), GROUPS), F32),
                pltpu.SemaphoreType.DMA((1,)),
                pltpu.SemaphoreType.DMA,
            ],
            compiler_params=pltpu.CompilerParams(vmem_limit_bytes=2**20),
        )(*(pltpu.with_memory_space_constraint(x, pltpu.VMEM) for x in found))
        return coeffs, mass.T

    specs = P("row", "col", None)
    return jax.shard_map(
        shards, mesh=mesh, in_specs=(specs,) * 3, out_specs=(specs, P()), check_vma=False
    )
```

```python
import functools

import jax
import jax.numpy as jnp
import numpy as np
from jax import lax
from jax.experimental import pallas as pl
from jax.experimental.pallas import tpu as pltpu
from jax.sharding import PartitionSpec as P

GROUPS = 16
LEVELS = (0.25, 0.5, 1.0, 2.0)
MESH = pl.DeviceIdType.MESH
F32, BF16 = jnp.float32, jnp.bfloat16
TILE, LANES = 8, 128
UNROLL = 64


def cyclic_matrix(n):
    ev, od = np.eye(n)[0::2], np.eye(n)[1::2]
    r = lambda a, k: np.roll(a, k, 0)
    d = od - (0.5625 * (ev + r(ev, -1)) - 0.0625 * (r(ev, 1) + r(ev, -2)))
    s = ev + (0.28125 * (r(d, 1) + d) - 0.03125 * (r(d, 2) + r(d, -1)))
    return np.stack([s, d], 1).reshape(n, n)


def local_matrix(n):
    half = n // 2
    t = np.eye(n + 6)
    v, (a, b, c, f0, f1, g) = t[:n], t[n:]
    e = {j: v[2 * j] for j in range(half)}
    o = {j: v[2 * j + 1] for j in range(half)}
    e[-1], e[half], e[half + 1] = a, f0, f1
    d = {
        j: o[j] - 0.5625 * (e[j] + e[j + 1]) + 0.0625 * (e[j - 1] + e[j + 2])
        for j in range(half)
    }
    d[-1] = b - 0.5625 * e[0] + 0.0625 * e[1]
    d[-2] = c + 0.0625 * e[0]
    d[half] = g + 0.0625 * e[half - 1]
    out = np.zeros((n, n + 6))
    for j in range(half):
        out[2 * j] = e[j] + 0.28125 * (d[j - 1] + d[j]) - 0.03125 * (d[j - 2] + d[j + 1])
        out[2 * j + 1] = d[j]
    return out


def partials_low(row, n):
    a = row(n - 2)
    b = row(n - 1) - 0.5625 * a + 0.0625 * row(n - 4)
    c = row(n - 3) - 0.5625 * (row(n - 4) + a) + 0.0625 * row(n - 6)
    return a, b, c


def partials_high(row):
    f0, f1 = row(0), row(2)
    return f0, f1, row(1) - 0.5625 * (f0 + f1) + 0.0625 * row(4)


def split(value):
    hi = value.astype(BF16)
    return hi, (value - hi.astype(F32)).astype(BF16)


def dot2(left, right):
    dot = functools.partial(jnp.dot, preferred_element_type=F32)
    if left.dtype == BF16:
        hi, lo = split(right)
        return dot(left, hi) + dot(left, lo)
    hi, lo = split(left)
    return dot(hi, right) + dot(lo, right)


def dot_pair(left, right):
    return jnp.dot(left, jnp.concatenate(split(right), 0), preferred_element_type=F32)


def doublings(n_row, n_col):
    hops, known = [], 1
    while known < n_col // 2:
        hops.append((1, known))
        known *= 2
    known = 0
    while known < n_row // 2:
        hops.append((0, max(known, 1)))
        known += max(known, 1)
    return hops


def band(first_row, coefs):
    shape = (2 * TILE, LANES)
    lane = lax.broadcasted_iota(jnp.int32, shape, 1)
    far = jnp.abs(lane - lax.broadcasted_iota(jnp.int32, shape, 0) + first_row)
    value = jnp.zeros(shape, F32)
    for k, (even, odd) in enumerate(coefs):
        if even or odd:
            value = jnp.where(far == k, jnp.where(lane % 2 == 1, odd, even), value)
    return value.astype(BF16)


def inner_twice(n):
    shape = (n - 2 * TILE, 2 * n)
    row, cell = (lax.broadcasted_iota(jnp.int32, shape, axis) for axis in (0, 1))
    far = jnp.abs(cell % n - row - TILE)
    value = jnp.zeros(shape, F32)
    for k, (even, odd) in enumerate(coefficients(n)):
        value = jnp.where(far == k, jnp.where(row % 2 == 1, odd, even), value)
    return value.astype(BF16)


def coefficients(n):
    full = cyclic_matrix(n)
    return [(float(full[0, k]), float(full[1, 1 + k])) for k in range(7)]


def fill_cyclic(ref):
    n = ref.shape[0]
    coefs = coefficients(n)
    reach = len(coefs)
    made = {}
    for r in range(0, n, 2 * TILE):
        for c in range(0, n, LANES):
            off = (c - r + n // 2) % n - n // 2
            near = off - 2 * TILE < reach and off + LANES > -reach
            key = off if near else None
            if key not in made:
                made[key] = band(off, coefs) if near else jnp.zeros((2 * TILE, LANES), BF16)
            ref[pl.ds(r, 2 * TILE), pl.ds(c, LANES)] = made[key]


def kernel(n_row, n_col, grp, cut_hbm, map_hbm, p_ref, *refs):
    weights, refs = refs[:2], refs[2:]
    out_ref, mass_ref = refs[:2]
    ext, q, hs, yh, ch, su, u, part, slots, block_ref, wz_ref = refs[2:13]
    held = refs[13:15]
    wx_ref, wall_ref = held
    in_sem, w_sem, h_send, h_recv, g_sem, hop_sem, last_sem = refs[15:]
    nx, ny, nz = p_ref.shape
    half = nx // 2
    tall = grp * ny + 6 * grp
    wy_ref = wall_ref.at[pl.ds(0, tall)]
    wc_ref = wall_ref.at[pl.ds(tall, 12 * TILE), pl.ds(0, 12 * TILE)]
    wu_ref = wall_ref.at[pl.ds(tall + 12 * TILE, 2 * TILE * grp), pl.ds(0, 12 * grp)]
    devices = n_row * n_col
    row, col = lax.axis_index("row"), lax.axis_index("col")
    me = row * n_col + col
    away_r = lambda k: lax.rem(row + (k + n_row), n_row)
    away_c = lambda k: lax.rem(col + (k + n_col), n_col)
    up_r, dn_r, up_c, dn_c = away_r(1), away_r(-1), away_c(1), away_c(-1)

    barrier = pltpu.get_barrier_semaphore()
    top = n_row - 1
    at_first, at_last = row == 0, row == top

    def signal(sem, r, c):
        pl.semaphore_signal(sem, inc=1, device_id=(r, c), device_id_type=MESH)

    for r, c in ((dn_r, col), (row, up_c), (row, dn_c)):
        signal(barrier, r, c)
    pl.when(jnp.logical_not(at_last))(lambda: signal(barrier, row + 1, col))

    fetched = [
        pltpu.make_async_copy(src, dst, w_sem.at[i])
        for i, (src, dst) in enumerate(zip(weights, held, strict=True))
    ]
    odd_core = lax.rem(col, 2)

    def first_way(r):
        return lax.select(r == 0, 0, odd_core)

    ways = (first_way(row), 1 - first_way(row))
    needs = ((nx - 2, nx - 1, nx - 4, nx - 3, nx - 6), (0, 2, 1, 4))

    def take(at, i):
        return pltpu.make_async_copy(p_ref.at[at], ext.at[at], in_sem.at[i])

    def landed(ref, sem):
        pltpu.make_async_copy(ref, ref, sem).wait()

    head = lax.select(ways[0] == 0, needs[0][0], needs[1][0])
    head_copy = take(pl.ds(head, 1), 0)
    head_copy.start()
    fetched[0].start()
    for flip in range(2):
        for way in range(2):

            @pl.when(ways[flip] == way)
            def _():
                for plane in needs[way][1 - flip :]:
                    take(pl.ds(plane, 1), 1 + flip).start()

    loads = []
    mid = nx - 11
    starts = (5, 5 + mid // 3, 5 + 2 * (mid // 3), nx - 6)
    for at, end in (*zip(starts[:-1], starts[1:], strict=True), (3, 4), (nx - 5, nx - 4)):
        loads.append(take(pl.ds(at, end - at), 3))
    for copy in loads:
        copy.start()
    for fetch in fetched[1:]:
        fetch.start()
    for src, i in ((cut_hbm, 0), (map_hbm, 1)):
        pltpu.make_async_copy(src, block_ref.at[pl.ds(i, 1)], w_sem.at[2]).start()

    hops = doublings(n_row, n_col)

    def call(k):
        axis, far = hops[k]
        if axis:
            aim = ((row, away_c(far)), (row, away_c(-far)))
        else:
            aim = ((away_r(far), col), (away_r(-far), col))
        for to in aim:
            signal(hop_sem.at[k], *to)

    def relay(k):
        if k < len(hops):
            with jax.named_scope(f"r{k}"):
                pl.semaphore_wait(hop_sem.at[k], 2)
                if k + 1 < len(hops):
                    call(k + 1)

    def remote(i, j, src, dst, to):
        return pltpu.make_async_remote_copy(
            src_ref=src, dst_ref=dst, send_sem=h_send.at[i], recv_sem=h_recv.at[j],
            device_id=to, device_id_type=MESH,
        )

    def halo(piece, way):
        first, count = 0, 3
        if isinstance(piece, int) and piece in (0, 3):
            rows = pl.ds(TILE, ny - 2 * TILE)
            first, count = (1, 2) if piece else (0, 1)
            piece = 0
        else:
            rows = pl.ds(pl.multiple_of((piece - 1) * (ny - TILE), TILE), TILE)
        planes = lambda at: pl.ds(at + 3 * way + first, count)
        to = lax.rem(row + 1 + way * (n_row - 2), n_row)
        slot = piece if isinstance(piece, int) and piece == 0 else piece + way * (piece // 2)
        return remote(0, slot, yh.at[planes(0), rows], q.at[planes(nx), rows], (to, col))

    with jax.named_scope("wz"):
        alone = inner_twice(ny)
        fill_cyclic(wz_ref)
        su[:, pl.ds(nx + 6, TILE - 6), :] = jnp.zeros((6, TILE - 6, nz), F32)
    def call_first():
        pl.semaphore_wait(barrier, 4)
        signal(last_sem, 0, col)

    with jax.named_scope("barl"):
        pl.when(at_last)(call_first)

    def prepare(way, flip):
        landed(ext.at[pl.ds(0, len(needs[way]) - 1 + flip)], in_sem.at[1 + flip])
        made = (partials_low, partials_high)[way]
        planes = made(lambda i: ext[i], *((nx,) if way == 0 else ()))
        for i, plane in enumerate(planes):
            hs[3 * way + i] = plane

    inside = ny - 2 * TILE
    inner_rows = pl.ds(TILE, inside)
    outer_rows = (pl.ds(0, TILE), pl.ds(ny - TILE, TILE))
    plane_rows = lambda way: hs[pl.ds(3 * way, 3)].reshape(3 * ny, nz)

    def lift_inner(way, data, first):
        count = 3 - first
        made = dot_pair(wx_ref[pl.ds(first * inside, count * inside)], data)
        yh[pl.ds(3 * way + first, count), inner_rows, :] = made.reshape(count, inside, nz)

    def lift_outer(way, data):
        made = dot_pair(wx_ref[pl.ds(3 * inside, 6 * TILE)], data).reshape(3, 2 * TILE, nz)
        for k, rows in enumerate(outer_rows):
            yh[pl.ds(3 * way, 3), rows, :] = made[:, k * TILE : (k + 1) * TILE, :]

    with jax.named_scope("hs0"):
        head_copy.wait()
    with jax.named_scope("lift0"):
        yh[3 * ways[0], inner_rows, :] = dot_pair(alone, ext[head])
    with jax.named_scope("bar"):
        pl.when(at_first)(lambda: pl.semaphore_wait(barrier, 3))
        pl.when(jnp.logical_not(at_first | at_last))(lambda: pl.semaphore_wait(barrier, 4))
    halo(0, ways[0]).start()
    with jax.named_scope("lift0b"):
        for way in range(2):
            pl.when(ways[0] == way)(lambda: prepare(way, 0))
        fetched[0].wait()
        lift_inner(ways[0], plane_rows(ways[0]), 1)
    halo(3, ways[0]).start()
    with jax.named_scope("hs1"):
        for way in range(2):
            pl.when(ways[1] == way)(lambda: prepare(way, 1))
        for i in range(6):
            line = lambda j: hs[i, pl.ds(j, 1), :]
            for k, one in enumerate(partials_low(line, ny) + partials_high(line)):
                su[k, pl.ds(nx + i, 1), :] = one
    lo, hi = pl.ds(0, 3), pl.ds(3, 3)
    for half_k, c in ((lo, up_c), (hi, dn_c)):
        remote(1, 4, su.at[half_k, pl.ds(nx, TILE)], ch.at[half_k], (row, c)).start()
    if hops:
        call(0)
    with jax.named_scope("lift1"):
        lifted = dot2(plane_rows(ways[1]), wz_ref[...])
        lift_inner(ways[1], lifted, 0)

    def second():
        halo(0, ways[1]).start()
        halo(3, ways[1]).start()

    pl.when(jnp.logical_not(at_first))(second)

    far = lax.select(at_first, 1, lax.select(at_last, 0, odd_core))
    tail = (
        (1, far + odd_core - 2 * far * odd_core), (2 - odd_core, far),
        (1 + odd_core, odd_core * far + (1 - odd_core) * (1 - far)), (2, 1 - far),
    )
    groups = nx // grp
    order = (0, groups - 1, *range(1, groups - 1))

    def z_group(g):
        at = pl.ds(g * grp, grp)
        v = dot2(ext[at].reshape(grp * ny, nz), wz_ref[...])
        got = dot2(wy_ref[...], v)
        q[at] = got[: grp * ny].reshape(grp, ny, nz)
        su[:, at, :] = got[grp * ny :].reshape(6, grp, nz)
        for half_k, c in ((lo, up_c), (hi, dn_c)):
            remote(1, 5 + (g == order[-1]), su.at[half_k, at], u.at[half_k, at], (row, c)).start()

    with jax.named_scope("ld2"):
        landed(ext.at[pl.ds(0, nx - len(sum(needs, ())))], in_sem.at[3])
        for fetch in fetched[1:]:
            fetch.wait()
        landed(block_ref, w_sem.at[2])
    with jax.named_scope("z"):
        for g in order[: groups // 2]:
            z_group(g)
    with jax.named_scope("last"):

        @pl.when(at_first)
        def _():
            pl.semaphore_wait(last_sem, 1)
            second()

    with jax.named_scope("lift2"):
        lift_outer(ways[1], lifted)
        lift_outer(ways[0], dot2(plane_rows(ways[0]), wz_ref[...]))
    relay(0)
    with jax.named_scope("z2"):
        z_group(order[groups // 2])
    with jax.named_scope("wait_corner"):
        landed(ch, h_recv.at[4])
    with jax.named_scope("outer"):
        lifted = dot2(ch[...].reshape(6 * TILE, nz), wz_ref[...])
        more = dot_pair(wc_ref[...], lifted).reshape(6, 2 * TILE, nz)
        for k, rows in enumerate(outer_rows):
            yh[:, rows, :] += more[:, k * TILE : (k + 1) * TILE, :]
        for piece, way in tail[:3]:
            halo(piece, way).start()
        last_piece = halo(*tail[3])
        pl.when(odd_core == 0)(last_piece.start)
    with jax.named_scope("z3"):
        for g in order[groups // 2 + 1 :]:
            z_group(g)
    relay(1)

    zb = block_ref.shape[2]
    width = nz // zb
    n_lev = len(LEVELS)
    odd = lambda axis: lax.broadcasted_iota(jnp.int32, (TILE, LANES), axis) % 2
    mixed = (odd(0) + odd(1)) > 0

    def x_stage(totals, edges, first, last, sides=(1, 0)):
        totals = list(totals)
        for z in range(zb):
            cuts = jnp.full((TILE, LANES), -block_ref[0, 0, z], jnp.int32)
            scale = jnp.exp2(cuts.astype(F32))
            limits = [level * scale for level in LEVELS]

            def tile(t, sums, z=z, limits=limits):
                rows = pl.ds(pl.multiple_of(t * TILE, TILE), TILE)
                sums = list(sums)
                for at in range(z * width, (z + 1) * width, LANES):
                    lanes = pl.ds(at, LANES)

                    def put(plane, value):
                        out_ref[plane, rows, lanes] = value
                        size = jnp.abs(value)
                        if plane % 2 == 0:
                            size = jnp.where(mixed, size, 0.0)
                        for n, limit in enumerate(limits):
                            sums[n] += jnp.maximum(size - limit, 0.0)

                    far = {-1: nx, half: nx + 3, half + 1: nx + 4}
                    e = lambda j: q[far.get(j, 2 * j), rows, lanes]

                    def detail(j):
                        if j == -1:
                            return q[nx + 1, rows, lanes] - 0.5625 * e(0) + 0.0625 * e(1)
                        if j == -2:
                            return q[nx + 2, rows, lanes] + 0.0625 * e(0)
                        if j == half:
                            return q[nx + 5, rows, lanes] + 0.0625 * e(half - 1)
                        return q[2 * j + 1, rows, lanes] - 0.5625 * (e(j) + e(j + 1)) + 0.0625 * (e(j - 1) + e(j + 2))

                    def smooth(d, j):
                        put(2 * j, e(j) + 0.28125 * (d[j - 1] + d[j]) - 0.03125 * (d[j - 2] + d[j + 1]))

                    if not edges:
                        d = {}
                        for j in range(1, half - 2):
                            d[j] = detail(j)
                            put(2 * j + 1, d[j])
                            if j >= 4:
                                smooth(d, j - 1)
                    if edges and 0 in sides:
                        d = {j: out_ref[2 * j + 1, rows, lanes] for j in (1, 2, 3)}
                        d |= {j: detail(j) for j in (-2, -1, 0)}
                        put(1, d[0])
                        for j in (0, 1, 2):
                            smooth(d, j)
                    if edges and 1 in sides:
                        d = {j: out_ref[2 * j + 1, rows, lanes] for j in range(half - 5, half - 2)}
                        d |= {j: detail(j) for j in range(half - 2, half + 1)}
                        for j in (half - 2, half - 1):
                            put(2 * j + 1, d[j])
                        for j in range(half - 3, half):
                            smooth(d, j)
                return tuple(sums)

            mine = slice(z * n_lev, (z + 1) * n_lev)
            totals[mine] = lax.fori_loop(first, last, tile, tuple(totals[mine]))
        return totals

    tiles = ny // TILE
    totals = [jnp.zeros((TILE, LANES), F32) for _ in range(zb * n_lev)]
    with jax.named_scope("xin"):
        totals = x_stage(totals, False, 1, tiles - 1)
    relay(2)
    with jax.named_scope("wait_inner"):
        landed(q.at[pl.ds(nx, 6), inner_rows], h_recv.at[0])

        def make_up(way):
            at = pl.ds(nx + 3 * way, 3)
            raw = q[at, inner_rows, :].reshape(3 * inside, nz)
            q[at, inner_rows, :] = dot2(raw, wz_ref[...]).reshape(3, inside, nz)

        pl.when(first_way(dn_r) == 0)(lambda: make_up(0))
        pl.when(first_way(up_r) == 1)(lambda: make_up(1))
    with jax.named_scope("xinner"):
        totals = x_stage(totals, True, 1, tiles - 1)
    for g in order:
        with jax.named_scope("wait_u"):
            if g in (order[0], order[-1]):
                count = 1 if g == order[-1] else groups - 1
                landed(u.at[:, pl.ds(0, count * grp)], h_recv.at[6 - (count > 1)])
        with jax.named_scope("u"):
            at = pl.ds(g * grp, grp)
            more = dot_pair(wu_ref[...], u[:, at, :].reshape(6 * grp, nz))
            more = more.reshape(grp, 2 * TILE, nz)
            for k, rows in enumerate(outer_rows):
                q[at, rows, :] += more[:, k * TILE : (k + 1) * TILE, :]
    pl.when(odd_core == 1)(lambda: halo(*tail[3]).start())
    for k in range(3, len(hops)):
        relay(k)
    with jax.named_scope("xin2"):
        for t in (0, tiles - 1):
            totals = x_stage(totals, False, t, t + 1)
    with jax.named_scope("wait_outer"):
        landed(q.at[pl.ds(nx, 6), outer_rows[0]], h_recv.at[1])
    with jax.named_scope("xouter"):
        totals = x_stage(totals, True, 0, 1)
    for way in (1, 0):
        with jax.named_scope("wait_outer"):
            landed(q.at[pl.ds(nx + 3 * way, 3), outer_rows[1]], h_recv.at[2 + way])
        with jax.named_scope("xouter"):
            totals = x_stage(totals, True, tiles - 1, tiles, (way,))
    with jax.named_scope("line"):
        rows = zb * n_lev
        lane, at = (lax.broadcasted_iota(jnp.int32, (rows, LANES), axis) for axis in (1, 0))
        group = jnp.full((rows, LANES), block_ref[1, 0, 0], jnp.int32)
        for z in range(1, zb):
            group = jnp.where(at >= z * n_lev, block_ref[1, 0, z], group)
        sums = jnp.concatenate([jnp.sum(total, axis=0, keepdims=True) for total in totals], 0)
        mass = jnp.sum(sums, axis=1, keepdims=True) / (nx * ny * width)
        line = jnp.where(lane == at % n_lev * GROUPS + group, mass, 0.0)
        line = jnp.sum(line, axis=0, keepdims=True)
        part[...] = line
        slots[me] = line

    def spread(r, c):
        pltpu.make_async_remote_copy(
            src_ref=part, dst_ref=slots.at[me], send_sem=g_sem.at[0],
            recv_sem=g_sem.at[1], device_id=(r, c), device_id_type=MESH,
        ).start()

    def peers(visit):
        if devices <= UNROLL:
            for j in (*range(1, n_row), 0):
                for k in range(n_col):
                    if j or k:
                        visit(away_r(j), away_c(k))
            return

        @pl.loop(1, n_row)
        def _(j):
            @pl.loop(0, n_col)
            def _(k):
                visit(lax.rem(row + j, n_row), lax.rem(col + k, n_col))

        @pl.loop(1, n_col)
        def _(k):
            visit(row, lax.rem(col + k, n_col))

    with jax.named_scope("spread"):
        peers(spread)
    with jax.named_scope("wsend"):
        for i, sent in enumerate((yh, su)):
            landed(sent, h_send.at[i])
    with jax.named_scope("gather"):
        for i in range(2):
            landed(slots.at[pl.ds(0, devices - 1)], g_sem.at[i])
    mass_ref[...] = slots[...]


def deliver(c_ref, m_ref, out_hbm, mass_hbm, mass, sems, m_sem):
    count = sems.shape[0]
    size = c_ref.shape[0] // count
    copies = []
    for i in range(count):
        at = pl.ds(i * size, size)
        copies.append(pltpu.make_async_copy(c_ref.at[at], out_hbm.at[at], sems.at[i]))
        copies[i].start()
    total = jnp.sum(m_ref[...], axis=0)
    mass[...] = jnp.concatenate(
        [total[:, n * GROUPS : (n + 1) * GROUPS] for n in range(len(LEVELS))], 0
    )
    copies.append(pltpu.make_async_copy(mass, mass_hbm, m_sem))
    copies[-1].start()
    for copy in copies:
        copy.wait()


def solution(mesh):
    n_row, n_col = mesh.shape["row"], mesh.shape["col"]

    def shards(pressure, cut_exponent, group_map):
        nx, ny, nz = pressure.shape
        grp = 8
        devices = n_row * n_col
        local = local_matrix(ny)
        own, beyond = local[:, :ny], local[:, ny:]
        eye = np.eye(ny)
        take = lambda i: eye[i]
        near = np.stack(partials_low(take, ny) + partials_high(take))
        ws = np.einsum("ky,xw->kxwy", near, np.eye(grp)).reshape(6 * grp, grp * ny)
        wy = np.concatenate([np.kron(np.eye(grp), own), ws])
        rim = np.r_[0:TILE, ny - TILE : ny]
        spread = lambda planes: np.einsum("wp,yk->pykw", planes, beyond[rim]).reshape(
            planes.shape[1] * 2 * TILE, -1
        )
        core = np.r_[TILE : ny - TILE]
        twice = lambda w: np.tile(w, 2)
        wx = np.concatenate([twice(np.kron(np.eye(3), own[rows])) for rows in (core, rim)])
        wc, wu = spread(np.eye(TILE, 6)), spread(np.eye(grp))
        wide = lambda w: np.pad(w, ((0, 0), (0, wy.shape[1] - w.shape[1])))
        wall = np.concatenate([wy, wide(twice(wc)), wide(twice(wu))])
        weights = [jnp.asarray(w, BF16) for w in (wx, wall)]
        vmem = pl.BlockSpec(memory_space=pltpu.VMEM)
        hbm = pl.BlockSpec(memory_space=pltpu.HBM)
        hops = len(doublings(n_row, n_col))
        found = pl.pallas_call(
            functools.partial(kernel, n_row, n_col, grp),
            out_shape=(
                pltpu.VMEM((nx, ny, nz), F32),
                pltpu.VMEM((devices, 1, LANES), F32),
            ),
            in_specs=[hbm] * (3 + len(weights)),
            out_specs=(vmem, vmem),
            scratch_shapes=[
                pltpu.VMEM((nx, ny, nz), F32),
                pltpu.VMEM((nx + 6, ny, nz), F32),
                pltpu.VMEM((6, ny, nz), F32),
                pltpu.VMEM((6, ny, nz), F32),
                pltpu.VMEM((6, TILE, nz), F32),
                pltpu.VMEM((6, nx + TILE, nz), F32),
                pltpu.VMEM((6, nx, nz), F32),
                pltpu.VMEM((1, LANES), F32),
                pltpu.VMEM((devices, 1, LANES), F32),
                pltpu.SMEM((2, *cut_exponent.shape[1:]), jnp.int32),
                pltpu.VMEM((nz, nz), BF16),
                *(pltpu.VMEM(w.shape, BF16) for w in weights),
                pltpu.SemaphoreType.DMA((4,)),
                pltpu.SemaphoreType.DMA((len(weights) + 1,)),
                pltpu.SemaphoreType.DMA((2,)),
                pltpu.SemaphoreType.DMA((7,)),
                pltpu.SemaphoreType.DMA((2,)),
                pltpu.SemaphoreType.REGULAR((max(hops, 1),)),
                pltpu.SemaphoreType.REGULAR,
            ],
            compiler_params=pltpu.CompilerParams(
                collective_id=0, has_side_effects=True, vmem_limit_bytes=24 * 2**20
            ),
        )(*(pltpu.with_memory_space_constraint(x, pltpu.HBM) for x in (cut_exponent, group_map, pressure, *weights)))
        coeffs, mass = pl.pallas_call(
            deliver,
            out_shape=(
                pltpu.HBM((nx, ny, nz), F32), pltpu.HBM((len(LEVELS), GROUPS), F32),
            ),
            in_specs=[vmem] * 2,
            out_specs=(hbm, hbm),
            scratch_shapes=[
                pltpu.VMEM((len(LEVELS), GROUPS), F32),
                pltpu.SemaphoreType.DMA((1,)),
                pltpu.SemaphoreType.DMA,
            ],
            compiler_params=pltpu.CompilerParams(vmem_limit_bytes=2**20),
        )(*(pltpu.with_memory_space_constraint(x, pltpu.VMEM) for x in found))
        return coeffs, mass.T

    specs = P("row", "col", None)
    return jax.shard_map(
        shards, mesh=mesh, in_specs=(specs,) * 3, out_specs=(specs, P()), check_vma=False
    )
```
